32 devices in a mesh: trial: 4 (over x, core), shard: 4 (over z), tp: 2 (over y).
Axes of the slice: x: 2, y: 2, z: 4, core: 2. Of those that a mesh axis runs over, the one named last changes fastest.
Arguments:
- weight_query: bfloat16 [10240, 4096], P(('trial', 'shard'), 'tp'), parts along dimension 0, may hold values from -0.125 to 0.125
- low_query: bfloat16 [10240, 64], P(('trial', 'shard')), parts along dimension 0, may hold values from -0.125 to 0.125
- high_query: bfloat16 [256, 4096], P('trial', 'tp'), parts along dimension 0, may hold values from -0.75 to 0.75
- weight_key: bfloat16 [10240, 1024], P(('trial', 'shard'), 'tp'), parts along dimension 0, may hold values from -0.125 to 0.125
- low_key: bfloat16 [10240, 64], P(('trial', 'shard')), parts along dimension 0, may hold values from -0.125 to 0.125
- high_key: bfloat16 [256, 1024], P('trial', 'tp'), parts along dimension 0, may hold values from -0.75 to 0.75
- weight_value: bfloat16 [10240, 1024], P(('trial', 'shard'), 'tp'), parts along dimension 0, may hold values from -0.125 to 0.125
- low_value: bfloat16 [10240, 64], P(('trial', 'shard')), parts along dimension 0, may hold values from -0.125 to 0.125
- high_value: bfloat16 [256, 1024], P('trial', 'tp'), parts along dimension 0, may hold values from -0.75 to 0.75
- norm_train: float32 [10240], P(('trial', 'shard', 'tp')), parts along dimension 0, may hold values from 0.25 to 1.75
- norm_step: float32 [10240], P(('trial', 'shard', 'tp')), parts along dimension 0, may hold values from -0.3 to 0.3
Outputs:
- serve_query: bfloat16 [16384, 2560], P(('trial', 'tp')), parts along dimension 0
- serve_key: bfloat16 [4096, 2560], P(('trial', 'tp')), parts along dimension 0
- serve_value: bfloat16 [4096, 2560], P(('trial', 'tp')), parts along dimension 0
- serve_norm: bfloat16 [10240], P('trial'), parts along dimension 0
The draws below stay inside these ranges and needn't reach their ends.
There are 4 independent parts, one for each index of `trial`. The reference program is written for one: setup_inputs(seed, part) draws one part's arguments, and reference() takes and returns one part's arrays. A program takes and returns all parts, laid end to end along the dimension named above; each array names one. Nothing has to cross between parts.
All inputs are finite; a program needn't handle non-finite values.
Results may differ from the reference program's by a relative error of at most 0.001.
Values may be sent and summed in bfloat16 or wider, within the bound.
No kernel may reach another device: no remote copies, remote signals or barrier semaphores. Data moves between devices by JAX's collectives and lax.ppermute only.
A program may use at most 128 MiB of HBM per device.

```python
import jax
import jax.numpy as jnp

D_MODEL = 2560
Q_DIM = 4096
KV_DIM = 1024
RANK = 64


def levels(stream_key, shape, split, low, top_value):
    factor_of = 1.0
    for dim, parts in split:
        steps = jax.random.uniform(jax.random.fold_in(jax.random.fold_in(stream_key, 6), dim), (parts,), jnp.float32, low / len(split), top_value / len(split))
        factor_of = factor_of * jnp.repeat(jnp.exp(steps), shape[dim] // parts).reshape((-1,) + (1,) * (len(shape) - 1 - dim))
    return factor_of


def normal_values(key, dims, scale, reach, split=(), dtype=jnp.bfloat16):
    level = levels(key, dims, split, -0.22, 0.18) if split else 1.0
    entries = jax.random.normal(key, dims, jnp.float32) * scale * level
    return jnp.minimum(jnp.maximum(entries, -reach), reach).astype(dtype)


def setup_inputs(seed: int = 0, part: int = 0) -> dict:
    keys = jax.random.split(jax.random.key(seed), 12)
    own_keys = jax.random.split(jax.random.fold_in(keys[11], part), 12)
    weight_query = normal_values(own_keys[0], (D_MODEL, Q_DIM), D_MODEL ** -0.5, 0.125, ((0, 4), (1, 2)))
    low_query = normal_values(own_keys[1], (D_MODEL, RANK), D_MODEL ** -0.5, 0.125, ((0, 4),))
    high_query = normal_values(own_keys[2], (RANK, Q_DIM), RANK ** -0.5, 0.75, ((1, 2),))
    weight_key = normal_values(own_keys[3], (D_MODEL, KV_DIM), D_MODEL ** -0.5, 0.125, ((0, 4), (1, 2)))
    low_key = normal_values(own_keys[4], (D_MODEL, RANK), D_MODEL ** -0.5, 0.125, ((0, 4),))
    high_key = normal_values(own_keys[5], (RANK, KV_DIM), RANK ** -0.5, 0.75, ((1, 2),))
    weight_value = normal_values(own_keys[6], (D_MODEL, KV_DIM), D_MODEL ** -0.5, 0.125, ((0, 4), (1, 2)))
    low_value = normal_values(own_keys[7], (D_MODEL, RANK), D_MODEL ** -0.5, 0.125, ((0, 4),))
    high_value = normal_values(own_keys[8], (RANK, KV_DIM), RANK ** -0.5, 0.75, ((1, 2),))
    norm_train = jnp.clip(1.0 + 0.15 * jax.random.normal(own_keys[9], (D_MODEL,), jnp.float32), 0.25, 1.75)
    norm_step = jnp.clip(jax.random.uniform(own_keys[10], (D_MODEL,), jnp.float32, -0.3, 0.3) * levels(own_keys[10], (D_MODEL,), ((0, 8),), -0.4, 0.0), -0.3, 0.3)
    return dict(weight_query=weight_query, low_query=low_query, high_query=high_query, weight_key=weight_key, low_key=low_key, high_key=high_key, weight_value=weight_value, low_value=low_value, high_value=high_value, norm_train=norm_train, norm_step=norm_step)


mix_rate = 1.0


def reference(weight_query, low_query, high_query, weight_key, low_key, high_key, weight_value, low_value, high_value, norm_train, norm_step):
    fresh_query = weight_query.astype(jnp.float32) + mix_rate * jnp.dot(low_query, high_query, preferred_element_type=jnp.float32)
    fresh_key = weight_key.astype(jnp.float32) + mix_rate * jnp.dot(low_key, high_key, preferred_element_type=jnp.float32)
    fresh_value = weight_value.astype(jnp.float32) + mix_rate * jnp.dot(low_value, high_value, preferred_element_type=jnp.float32)
    serve_query = fresh_query.T.astype(jnp.bfloat16)
    serve_key = fresh_key.T.astype(jnp.bfloat16)
    serve_value = fresh_value.T.astype(jnp.bfloat16)
    serve_norm = (norm_train + norm_step).astype(jnp.bfloat16)
    return serve_query, serve_key, serve_value, serve_norm
```

```python
import functools

import jax
import jax.numpy as jnp
from jax import lax
from jax.experimental import pallas as pl
from jax.experimental.pallas import tpu as pltpu
from jax.sharding import PartitionSpec as P

mix_rate = 1.0


def merge_kernel(me_ref, weight_ref, low_ref, high_ref, *rest):
    chunk_ref, out_ref = rest[-2:]
    delta = lax.dot_general(
        high_ref[...], low_ref[...], (((0,), (0,)), ((), ())), preferred_element_type=jnp.float32
    )
    fresh = weight_ref[...].T.astype(jnp.float32) + mix_rate * delta
    fresh = fresh.astype(jnp.bfloat16)
    chunk_ref[...] = fresh
    out_ref[...] = fresh


def merge_chunk(me, weight, low_t, high, out, start, rows, block, total):
    depth, columns = weight.shape
    rank = high.shape[0]
    first = start // block
    in_specs = [
        pl.BlockSpec((depth, block), lambda j, me: (0, first + j)),
        pl.BlockSpec((rank, depth), lambda j, me: (0, 0)),
        pl.BlockSpec((rank, block), lambda j, me: (0, first + j)),
    ]
    operands = [weight, low_t, high]
    aliases = {}
    if out is not None:
        in_specs.append(pl.BlockSpec(memory_space=pl.ANY))
        operands.append(out)
        aliases = {4: 1}
    return pl.pallas_call(
        merge_kernel,
        grid_spec=pltpu.PrefetchScalarGridSpec(
            num_scalar_prefetch=1,
            grid=(rows // block,),
            in_specs=in_specs,
            out_specs=[
                pl.BlockSpec((block, depth), lambda j, me: (j, 0)),
                pl.BlockSpec((block, depth), lambda j, me: (first + j, me[0])),
            ],
        ),
        out_shape=[
            jax.ShapeDtypeStruct((rows, depth), jnp.bfloat16),
            jax.ShapeDtypeStruct((columns, total), jnp.bfloat16),
        ],
        input_output_aliases=aliases,
        cost_estimate=pl.CostEstimate(
            flops=2 * rows * depth * rank, bytes_accessed=6 * rows * depth, transcendentals=0
        ),
        name="merge",
    )(me, *operands)


def place_kernel(start, rows, depth, pieces, where_ref, chunk_ref, _, out_ref, tiles, in_sem, out_sem):
    step = rows // pieces

    @pl.when(where_ref[0] == 1)
    def _():
        column = pl.multiple_of(where_ref[1] * depth, 128)
        ins, outs = [], []
        for p in range(pieces):
            part = pl.ds(p * step, step)
            ins.append(pltpu.make_async_copy(chunk_ref.at[part], tiles.at[part], in_sem.at[p]))
            outs.append(
                pltpu.make_async_copy(
                    tiles.at[part],
                    out_ref.at[pl.ds(start + p * step, step), pl.ds(column, depth)],
                    out_sem.at[p],
                )
            )
        for copy in ins:
            copy.start()
        for p in range(pieces):
            ins[p].wait()
            outs[p].start()
        for copy in outs:
            copy.wait()


def place_chunk(where, chunk, out, start, pieces=2):
    rows, depth = chunk.shape
    return pl.pallas_call(
        functools.partial(place_kernel, start, rows, depth, pieces),
        grid_spec=pltpu.PrefetchScalarGridSpec(
            num_scalar_prefetch=1,
            grid=(1,),
            in_specs=[pl.BlockSpec(memory_space=pl.ANY), pl.BlockSpec(memory_space=pl.ANY)],
            out_specs=pl.BlockSpec(memory_space=pl.ANY),
            scratch_shapes=[
                pltpu.VMEM((rows, depth), jnp.bfloat16),
                pltpu.SemaphoreType.DMA((pieces,)),
                pltpu.SemaphoreType.DMA((pieces,)),
            ],
        ),
        out_shape=jax.ShapeDtypeStruct(out.shape, out.dtype),
        input_output_aliases={2: 0},
        cost_estimate=pl.CostEstimate(
            flops=rows * depth, bytes_accessed=4 * rows * depth, transcendentals=0
        ),
        name="place",
    )(where, chunk, out)


def line_hops(n):
    hops = []
    for r in range(1, n):
        for parity in (0, 1):
            pairs = []
            for i in range(parity, n - 1, 2):
                if i - r + 1 >= 0:
                    pairs.append((i, i + 1))
                if i + r <= n - 1:
                    pairs.append((i + 1, i))
            if pairs:
                hops.append((r, parity, pairs))
    return hops


def gathered(arrays, norm_train, norm_step):
    serve = [
        lax.all_gather(
            (
                weight.astype(jnp.float32)
                + mix_rate * jnp.dot(low, high, preferred_element_type=jnp.float32)
            ).astype(jnp.bfloat16),
            "shard",
            axis=0,
            tiled=True,
        ).T
        for weight, low, high in arrays
    ]
    share = (norm_train + norm_step).astype(jnp.bfloat16)
    return (*serve, lax.all_gather(share, ("shard", "tp"), axis=0, tiled=True))


def solution(mesh):
    n, nt = mesh.shape["shard"], mesh.shape["tp"]

    def on_device(
        weight_query,
        low_query,
        high_query,
        weight_key,
        low_key,
        high_key,
        weight_value,
        low_value,
        high_value,
        norm_train,
        norm_step,
    ):
        if weight_query.shape[0] % 128:
            arrays = (
                (weight_query, low_query, high_query),
                (weight_key, low_key, high_key),
                (weight_value, low_value, high_value),
            )
            return gathered(arrays, norm_train, norm_step)
        me = lax.axis_index("shard")
        me_arr = jnp.reshape(me, (1,)).astype(jnp.int32)
        depth = weight_query.shape[0]
        total = depth * n
        weights = (weight_key, weight_query, weight_value)
        lows = (low_key.T, low_query.T, low_value.T)
        highs = (high_key, high_query, high_value)
        piece = weight_key.shape[1]
        plan = [
            (which, start, piece)
            for which in range(3)
            for start in range(0, weights[which].shape[1], piece)
        ]

        share = (norm_train + norm_step).astype(jnp.bfloat16)
        mine = lax.axis_index("tp")
        row = jnp.zeros((nt,) + share.shape, jnp.bfloat16)
        row = lax.dynamic_update_slice(row, share[None], (mine, 0))
        for k in range(1, nt):
            other = lax.ppermute(share, "tp", [(i, (i + k) % nt) for i in range(nt)])
            row = lax.dynamic_update_slice(row, other[None], ((mine + nt - k) % nt, 0))
        row = jnp.reshape(row, (-1,))

        outs = [None, None, None]
        chunks = []
        for which, start, rows in plan:
            block = min(rows, 128)
            chunk, outs[which] = merge_chunk(
                me_arr, weights[which], lows[which], highs[which], outs[which], start, rows, block, total
            )
            chunks.append(chunk)
            if len(chunks) == 1:
                chunks.append(row)
        plan.insert(1, None)
        norm = jnp.zeros((total,), jnp.bfloat16)
        norm = lax.dynamic_update_slice(norm, row, (me * depth,))

        even = me % 2 == 0
        last = {0: chunks, 1: chunks}
        for r in range(1, n):
            fresh = {}
            for rr, parity, pairs in line_hops(n):
                if rr != r:
                    continue
                held = last[1 - parity]
                source = jnp.where(even == (parity == 0), me + r, me - r)
                there = (source >= 0) & (source < n)
                where = jnp.stack([there.astype(jnp.int32), jnp.where(there, source, me)]).astype(jnp.int32)
                got = [lax.ppermute(c, "shard", pairs) for c in held]
                fresh[parity] = got
                for spot, chunk in zip(plan, got):
                    if spot is None:
                        offset = where[1] * depth
                        current = lax.dynamic_slice(norm, (offset,), (depth,))
                        norm = lax.dynamic_update_slice(norm, jnp.where(there, chunk, current), (offset,))
                    else:
                        which, start, _ = spot
                        outs[which] = place_chunk(where, chunk, outs[which], start)
            last = {0: fresh.get(0, chunks), 1: fresh.get(1, chunks)}
        serve_key, serve_query, serve_value = outs
        return serve_query, serve_key, serve_value, norm

    in_specs = (
        P(("trial", "shard"), "tp"),
        P(("trial", "shard"), None),
        P("trial", "tp"),
        P(("trial", "shard"), "tp"),
        P(("trial", "shard"), None),
        P("trial", "tp"),
        P(("trial", "shard"), "tp"),
        P(("trial", "shard"), None),
        P("trial", "tp"),
        P(("trial", "shard", "tp")),
        P(("trial", "shard", "tp")),
    )
    out_specs = (
        P(("trial", "tp"), None),
        P(("trial", "tp"), None),
        P(("trial", "tp"), None),
        P("trial"),
    )
    return jax.shard_map(
        on_device, mesh=mesh, in_specs=in_specs, out_specs=out_specs, check_vma=False
    )
```

```python
import functools

import jax
import jax.numpy as jnp
from jax import lax
from jax.experimental import pallas as pl
from jax.experimental.pallas import tpu as pltpu
from jax.sharding import PartitionSpec as P

mix_rate = 1.0


KEY, QUERY, VALUE = range(3)


def merge_kernel(me_ref, weight_ref, low_ref, high_ref, chunk_ref, out_ref):
    delta = lax.dot_general(
        high_ref[...], low_ref[...], (((0,), (0,)), ((), ())), preferred_element_type=jnp.float32
    )
    fresh = weight_ref[...].T.astype(jnp.float32) + mix_rate * delta
    fresh = fresh.astype(jnp.bfloat16)
    chunk_ref[...] = fresh
    out_ref[...] = fresh


def merge(me, weight, low_t, high, total):
    depth, columns = weight.shape
    rank = high.shape[0]
    block = next(b for b in (512, 256, 128, columns) if columns % b == 0)
    if columns == block and columns % 256 == 0:
        block = columns // 2
    return pl.pallas_call(
        merge_kernel,
        grid_spec=pltpu.PrefetchScalarGridSpec(
            num_scalar_prefetch=1,
            grid=(columns // block,),
            in_specs=[
                pl.BlockSpec((depth, block), lambda j, me: (0, j)),
                pl.BlockSpec((rank, depth), lambda j, me: (0, 0)),
                pl.BlockSpec((rank, block), lambda j, me: (0, j)),
            ],
            out_specs=[
                pl.BlockSpec((block, depth), lambda j, me: (j, 0)),
                pl.BlockSpec((block, depth), lambda j, me: (j, me[0])),
            ],
        ),
        out_shape=[
            jax.ShapeDtypeStruct((columns, depth), jnp.bfloat16),
            jax.ShapeDtypeStruct((columns, total), jnp.bfloat16),
        ],
        cost_estimate=pl.CostEstimate(
            flops=2 * columns * depth * rank, bytes_accessed=6 * columns * depth, transcendentals=0
        ),
        name="merge",
    )(me, weight, low_t, high)


def source_of(me, r, parity):
    down = lax.rem(me + parity, 2) == 0
    return jnp.where(down, me + r, me - r)


def place_kernel(n, r, parity, pieces, me_ref, chunk_ref, _, out_ref, tiles, in_sem, out_sem):
    rows, depth = chunk_ref.shape
    step = rows // pieces
    source = source_of(me_ref[0], r, parity)

    @pl.when((source >= 0) & (source < n))
    def _():
        column = pl.multiple_of(source * depth, 128)
        ins, outs = [], []
        for p in range(pieces):
            part = pl.ds(p * step, step)
            ins.append(pltpu.make_async_copy(chunk_ref.at[part], tiles.at[part], in_sem.at[p]))
            outs.append(
                pltpu.make_async_copy(
                    tiles.at[part], out_ref.at[part, pl.ds(column, depth)], out_sem.at[p]
                )
            )
        for copy in ins:
            copy.start()
        for p in range(pieces):
            ins[p].wait()
            outs[p].start()
        for copy in outs:
            copy.wait()


def place(me, n, r, parity, chunk, out):
    rows, depth = chunk.shape
    pieces = 4 if rows % 64 == 0 else 1
    return pl.pallas_call(
        functools.partial(place_kernel, n, r, parity, pieces),
        grid_spec=pltpu.PrefetchScalarGridSpec(
            num_scalar_prefetch=1,
            grid=(1,),
            in_specs=[pl.BlockSpec(memory_space=pl.ANY), pl.BlockSpec(memory_space=pl.ANY)],
            out_specs=pl.BlockSpec(memory_space=pl.ANY),
            scratch_shapes=[
                pltpu.VMEM((rows, depth), jnp.bfloat16),
                pltpu.SemaphoreType.DMA((pieces,)),
                pltpu.SemaphoreType.DMA((pieces,)),
            ],
        ),
        out_shape=jax.ShapeDtypeStruct(out.shape, out.dtype),
        input_output_aliases={2: 0},
        cost_estimate=pl.CostEstimate(
            flops=rows * depth, bytes_accessed=4 * rows * depth, transcendentals=0
        ),
        name="place",
    )(me, chunk, out)


def hop_pairs(n, r, parity):
    pairs = []
    for i in range(parity, n - 1, 2):
        if i - r + 1 >= 0:
            pairs.append((i, i + 1))
        if i + r <= n - 1:
            pairs.append((i + 1, i))
    return pairs


def steps_of(n):
    chunks = (KEY, QUERY, None, VALUE)
    steps = []
    for which in chunks:
        steps.append(("merge", 0, 0, which) if which is not None else ("exchange", 0, 0, None))
        for parity in (0, 1):
            if hop_pairs(n, 1, parity):
                steps.append(("hop", 1, parity, which))
    for r in range(2, n + 1):
        for which in chunks:
            for parity in (0, 1):
                if hop_pairs(n, r, parity):
                    steps.append(("hop", r, parity, which))
            if which is None:
                if r == n:
                    steps.append(("norm", 0, 0, None))
                continue
            for parity in (0, 1):
                if hop_pairs(n, r - 1, parity):
                    steps.append(("place", r - 1, parity, which))
    return steps


def gathered(arrays, norm_train, norm_step):
    serve = [
        lax.all_gather(
            (
                weight.astype(jnp.float32)
                + mix_rate * jnp.dot(low, high, preferred_element_type=jnp.float32)
            ).astype(jnp.bfloat16),
            "shard",
            axis=0,
            tiled=True,
        ).T
        for weight, low, high in arrays
    ]
    share = (norm_train + norm_step).astype(jnp.bfloat16)
    return (*serve, lax.all_gather(share, ("shard", "tp"), axis=0, tiled=True))


def solution(mesh):
    n, nt = mesh.shape["shard"], mesh.shape["tp"]
    steps = steps_of(n)

    def on_device(
        weight_query,
        low_query,
        high_query,
        weight_key,
        low_key,
        high_key,
        weight_value,
        low_value,
        high_value,
        norm_train,
        norm_step,
    ):
        depth = weight_query.shape[0]
        if depth % 128:
            arrays = (
                (weight_query, low_query, high_query),
                (weight_key, low_key, high_key),
                (weight_value, low_value, high_value),
            )
            return gathered(arrays, norm_train, norm_step)
        me = lax.axis_index("shard")
        me_ref = jnp.reshape(me, (1,)).astype(jnp.int32)
        mine = lax.axis_index("tp")
        inputs = {
            KEY: (weight_key, low_key.T, high_key),
            QUERY: (weight_query, low_query.T, high_query),
            VALUE: (weight_value, low_value.T, high_value),
        }
        outs = {}
        got = {}
        for what, r, parity, which in steps:
            if what == "merge":
                chunk, outs[which] = merge(me_ref, *inputs[which], depth * n)
                got[0, 0, which] = got[0, 1, which] = chunk
            elif what == "exchange":
                share = (norm_train + norm_step).astype(jnp.bfloat16)
                shares = [share] + [
                    lax.ppermute(share, "tp", [(j, (j + k) % nt) for j in range(nt)])
                    for k in range(1, nt)
                ]
                parts = []
                for j in range(nt):
                    part = share
                    for k in range(1, nt):
                        part = jnp.where(mine == (j + k) % nt, shares[k], part)
                    parts.append(part)
                got[0, 0, None] = got[0, 1, None] = jnp.concatenate(parts)
            elif what == "hop":
                held = got[r - 1, 1 - parity, which]
                got[r, parity, which] = lax.ppermute(held, "shard", hop_pairs(n, r, parity))
            elif what == "place":
                outs[which] = place(me_ref, n, r, parity, got[r, parity, which], outs[which])
            else:
                rows = []
                for s in range(n):
                    row = got[0, 0, None]
                    for (r, parity, which), value in got.items():
                        if which is None and r > 0:
                            row = jnp.where(source_of(me, r, parity) == s, value, row)
                    rows.append(row)
                serve_norm = jnp.concatenate(rows)
        return outs[QUERY], outs[KEY], outs[VALUE], serve_norm

    in_specs = (
        P(("trial", "shard"), "tp"),
        P(("trial", "shard"), None),
        P("trial", "tp"),
        P(("trial", "shard"), "tp"),
        P(("trial", "shard"), None),
        P("trial", "tp"),
        P(("trial", "shard"), "tp"),
        P(("trial", "shard"), None),
        P("trial", "tp"),
        P(("trial", "shard", "tp")),
        P(("trial", "shard", "tp")),
    )
    out_specs = (
        P(("trial", "tp"), None),
        P(("trial", "tp"), None),
        P(("trial", "tp"), None),
        P("trial"),
    )
    return jax.shard_map(
        on_device, mesh=mesh, in_specs=in_specs, out_specs=out_specs, check_vma=False
    )
```

```python
import functools

import jax
import jax.numpy as jnp
from jax import lax
from jax.experimental import pallas as pl
from jax.experimental.pallas import tpu as pltpu
from jax.sharding import PartitionSpec as P

mix_rate = 1.0


KEY, QUERY, VALUE = range(3)
FIRST, LAST, NORM = (KEY, 0, 4), (VALUE, 6, 2), None
KEY_REST, QUERY_ALL, VALUE_REST = (KEY, 4, 4), (QUERY, 0, 8), (VALUE, 0, 6)
CHUNKS = (FIRST, KEY_REST, QUERY_ALL, NORM, VALUE_REST, LAST)
EIGHTHS = 8


def merged(weight_ref, low_ref, high_ref):
    delta = lax.dot_general(
        high_ref[...], low_ref[...], (((0,), (0,)), ((), ())), preferred_element_type=jnp.float32
    )
    fresh = weight_ref[...].T.astype(jnp.float32) + mix_rate * delta
    return fresh.astype(jnp.bfloat16)


def first_kernel(weight_ref, low_ref, high_ref, chunk_ref):
    chunk_ref[...] = merged(weight_ref, low_ref, high_ref)


def merge_kernel(me_ref, weight_ref, low_ref, high_ref, *rest):
    chunk_ref, out_ref = rest[-2:]
    fresh = merged(weight_ref, low_ref, high_ref)
    chunk_ref[...] = fresh
    out_ref[...] = fresh


def extent(columns, chunk):
    return columns * chunk[1] // EIGHTHS, columns * chunk[2] // EIGHTHS


def cost(rows, depth, rank):
    return pl.CostEstimate(
        flops=2 * rows * depth * rank, bytes_accessed=6 * rows * depth, transcendentals=0
    )


def merge_first(weight, low_t, high, chunk):
    depth, columns = weight.shape
    rank = high.shape[0]
    start, rows = extent(columns, chunk)
    return pl.pallas_call(
        first_kernel,
        grid=(1,),
        in_specs=[
            pl.BlockSpec((depth, rows), lambda j: (0, start // rows)),
            pl.BlockSpec((rank, depth), lambda j: (0, 0)),
            pl.BlockSpec((rank, rows), lambda j: (0, start // rows)),
        ],
        out_specs=pl.BlockSpec(memory_space=pltpu.VMEM),
        out_shape=pltpu.VMEM((rows, depth), jnp.bfloat16),
        cost_estimate=cost(rows, depth, rank),
        name="merge",
    )(weight, low_t, high)


def merge(me, weight, low_t, high, chunk, out):
    depth, columns = weight.shape
    rank = high.shape[0]
    start, rows = extent(columns, chunk)
    block = next(b for b in (512, 256, 128) if start % b == 0 and rows % b == 0)
    first = start // block
    in_specs = [
        pl.BlockSpec((depth, block), lambda j, me: (0, first + j)),
        pl.BlockSpec((rank, depth), lambda j, me: (0, 0)),
        pl.BlockSpec((rank, block), lambda j, me: (0, first + j)),
    ]
    operands = [weight, low_t, high]
    aliases = {}
    if isinstance(out, jax.Array):
        in_specs.append(pl.BlockSpec(memory_space=pl.ANY))
        operands.append(out)
        aliases = {4: 1}
    return pl.pallas_call(
        merge_kernel,
        grid_spec=pltpu.PrefetchScalarGridSpec(
            num_scalar_prefetch=1,
            grid=(rows // block,),
            in_specs=in_specs,
            out_specs=[
                pl.BlockSpec((block, depth), lambda j, me: (j, 0)),
                pl.BlockSpec((block, depth), lambda j, me: (first + j, me[0])),
            ],
        ),
        out_shape=[
            jax.ShapeDtypeStruct((rows, depth), jnp.bfloat16),
            jax.ShapeDtypeStruct(out.shape, jnp.bfloat16),
        ],
        input_output_aliases=aliases,
        cost_estimate=cost(rows, depth, rank),
        name="merge",
    )(me, *operands)


def source_of(me, r, parity):
    down = lax.rem(me + parity, 2) == 0
    return jnp.where(down, me + r, me - r)


def place_kernel(n, r, parity, start, pieces, me_ref, chunk_ref, _, out_ref, out_sem, in_sem=None, tiles=None):
    rows, depth = chunk_ref.shape
    step = rows // pieces
    source = me_ref[0] if r == 0 else source_of(me_ref[0], r, parity)

    @pl.when((source >= 0) & (source < n))
    def _():
        column = pl.multiple_of(source * depth, 128)
        held = chunk_ref if tiles is None else tiles
        ins, outs = [], []
        for p in range(pieces):
            part = pl.ds(p * step, step)
            if tiles is not None:
                ins.append(pltpu.make_async_copy(chunk_ref.at[part], tiles.at[part], in_sem.at[p]))
            there = out_ref.at[pl.ds(start + p * step, step), pl.ds(column, depth)]
            outs.append(pltpu.make_async_copy(held.at[part], there, out_sem.at[p]))
        for copy in ins:
            copy.start()
        for p in range(pieces):
            if ins:
                ins[p].wait()
            outs[p].start()
        for copy in outs:
            copy.wait()


def place(me, n, r, parity, chunk, out, start, in_vmem):
    rows, depth = chunk.shape
    pieces = 1 if in_vmem or rows % 64 else 4
    scratch = [pltpu.SemaphoreType.DMA((pieces,))]
    if in_vmem:
        chunk = pltpu.with_memory_space_constraint(chunk, pltpu.VMEM)
    else:
        scratch += [pltpu.SemaphoreType.DMA((pieces,)), pltpu.VMEM((rows, depth), jnp.bfloat16)]
    return pl.pallas_call(
        functools.partial(place_kernel, n, r, parity, start, pieces),
        grid_spec=pltpu.PrefetchScalarGridSpec(
            num_scalar_prefetch=1,
            grid=(1,),
            in_specs=[
                pl.BlockSpec(memory_space=pltpu.VMEM if in_vmem else pl.ANY),
                pl.BlockSpec(memory_space=pl.ANY),
            ],
            out_specs=pl.BlockSpec(memory_space=pl.ANY),
            scratch_shapes=scratch,
        ),
        out_shape=jax.ShapeDtypeStruct(out.shape, out.dtype),
        input_output_aliases={2: 0},
        cost_estimate=pl.CostEstimate(
            flops=rows * depth, bytes_accessed=4 * rows * depth, transcendentals=0
        ),
        name="place",
    )(me, chunk, out)


def hop_pairs(n, r, parity):
    pairs = []
    for i in range(parity, n - 1, 2):
        if i - r + 1 >= 0:
            pairs.append((i, i + 1))
        if i + r <= n - 1:
            pairs.append((i + 1, i))
    return pairs


def steps_of(n):
    def hops(r, chunks, parities=(0, 1)):
        return [
            ("hop", r, parity, chunk)
            for parity in parities
            for chunk in chunks
            if hop_pairs(n, r, parity)
        ]

    steps = []
    early = (FIRST, KEY_REST, QUERY_ALL)
    late = (VALUE_REST, LAST)
    for chunk in early:
        steps.append(("merge", 0, 0, chunk))
        steps += hops(1, [chunk], [0])
    steps += hops(1, early, [1])
    steps.append(("place", 0, 0, FIRST))
    steps += [("merge", 0, 0, chunk) for chunk in late]
    steps += hops(1, late)
    steps.append(("exchange", 0, 0, NORM))
    steps += hops(1, [NORM])
    for r in range(2, n + 1):
        for chunk in CHUNKS:
            steps += hops(r, [chunk])
            if chunk is NORM:
                if r == n:
                    steps.append(("norm", 0, 0, NORM))
                continue
            for parity in (0, 1):
                if hop_pairs(n, r - 1, parity):
                    steps.append(("place", r - 1, parity, chunk))
    return steps


def gathered(arrays, norm_train, norm_step):
    serve = [
        lax.all_gather(
            (
                weight.astype(jnp.float32)
                + mix_rate * jnp.dot(low, high, preferred_element_type=jnp.float32)
            ).astype(jnp.bfloat16),
            "shard",
            axis=0,
            tiled=True,
        ).T
        for weight, low, high in arrays
    ]
    share = (norm_train + norm_step).astype(jnp.bfloat16)
    return (*serve, lax.all_gather(share, ("shard", "tp"), axis=0, tiled=True))


def solution(mesh):
    n, nt = mesh.shape["shard"], mesh.shape["tp"]
    steps = steps_of(n)

    def on_device(
        weight_query,
        low_query,
        high_query,
        weight_key,
        low_key,
        high_key,
        weight_value,
        low_value,
        high_value,
        norm_train,
        norm_step,
    ):
        depth = weight_query.shape[0]
        if depth % 128 or any(w.shape[1] % 512 for w in (weight_query, weight_key, weight_value)):
            arrays = (
                (weight_query, low_query, high_query),
                (weight_key, low_key, high_key),
                (weight_value, low_value, high_value),
            )
            return gathered(arrays, norm_train, norm_step)
        me = lax.axis_index("shard")
        me_ref = jnp.reshape(me, (1,)).astype(jnp.int32)
        mine = lax.axis_index("tp")
        inputs = {
            KEY: (weight_key, low_key.T, high_key),
            QUERY: (weight_query, low_query.T, high_query),
            VALUE: (weight_value, low_value.T, high_value),
        }
        outs = {}
        got = {}
        for what, r, parity, chunk in steps:
            if what == "merge":
                weight, low_t, high = inputs[chunk[0]]
                if chunk is FIRST:
                    piece = merge_first(weight, low_t, high, chunk)
                else:
                    shape = jax.ShapeDtypeStruct((weight.shape[1], depth * n), jnp.bfloat16)
                    out = outs.get(chunk[0], shape)
                    piece, outs[chunk[0]] = merge(me_ref, weight, low_t, high, chunk, out)
                got[0, 0, chunk] = got[0, 1, chunk] = piece
            elif what == "exchange":
                share = (norm_train + norm_step).astype(jnp.bfloat16)
                shares = [share] + [
                    lax.ppermute(share, "tp", [(j, (j + k) % nt) for j in range(nt)])
                    for k in range(1, nt)
                ]
                parts = []
                for j in range(nt):
                    part = share
                    for k in range(1, nt):
                        part = jnp.where(mine == (j + k) % nt, shares[k], part)
                    parts.append(part)
                got[0, 0, NORM] = got[0, 1, NORM] = jnp.concatenate(parts)
            elif what == "hop":
                held = got[r - 1, 1 - parity, chunk]
                got[r, parity, chunk] = lax.ppermute(held, "shard", hop_pairs(n, r, parity))
            elif what == "place":
                piece, out = got[r, parity, chunk], outs[chunk[0]]
                start, _ = extent(out.shape[0], chunk)
                in_vmem = r == 0 or (r == n - 1 and chunk[0] == VALUE)
                outs[chunk[0]] = place(me_ref, n, r, parity, piece, out, start, in_vmem)
            else:
                rows = []
                for s in range(n):
                    row = got[0, 0, NORM]
                    for (r, parity, chunk), value in got.items():
                        if chunk is NORM and r > 0:
                            row = jnp.where(source_of(me, r, parity) == s, value, row)
                    rows.append(row)
                serve_norm = jnp.concatenate(rows)
        return outs[QUERY], outs[KEY], outs[VALUE], serve_norm

    in_specs = (
        P(("trial", "shard"), "tp"),
        P(("trial", "shard"), None),
        P("trial", "tp"),
        P(("trial", "shard"), "tp"),
        P(("trial", "shard"), None),
        P("trial", "tp"),
        P(("trial", "shard"), "tp"),
        P(("trial", "shard"), None),
        P("trial", "tp"),
        P(("trial", "shard", "tp")),
        P(("trial", "shard", "tp")),
    )
    out_specs = (
        P(("trial", "tp"), None),
        P(("trial", "tp"), None),
        P(("trial", "tp"), None),
        P("trial"),
    )
    return jax.shard_map(
        on_device, mesh=mesh, in_specs=in_specs, out_specs=out_specs, check_vma=False
    )
```

```python
import functools

import jax
import jax.numpy as jnp
from jax import lax
from jax.experimental import pallas as pl
from jax.experimental.pallas import tpu as pltpu
from jax.sharding import PartitionSpec as P

mix_rate = 1.0


KEY, QUERY, VALUE = range(3)
FIRST, LAST, NORM = KEY, VALUE, None
CHUNKS = (KEY, QUERY, NORM, VALUE)


def merged(weight_ref, low_ref, high_ref):
    delta = lax.dot_general(
        high_ref[...], low_ref[...], (((0,), (0,)), ((), ())), preferred_element_type=jnp.float32
    )
    fresh = weight_ref[...].T.astype(jnp.float32) + mix_rate * delta
    return fresh.astype(jnp.bfloat16)


def first_kernel(weight_ref, low_ref, high_ref, chunk_ref):
    chunk_ref[...] = merged(weight_ref, low_ref, high_ref)


def merge_kernel(me_ref, weight_ref, low_ref, high_ref, chunk_ref, out_ref):
    fresh = merged(weight_ref, low_ref, high_ref)
    chunk_ref[...] = fresh
    out_ref[...] = fresh


def cost(rows, depth, rank):
    return pl.CostEstimate(
        flops=2 * rows * depth * rank, bytes_accessed=6 * rows * depth, transcendentals=0
    )


def merge_first(weight, low_t, high):
    depth, columns = weight.shape
    rank = high.shape[0]
    return pl.pallas_call(
        first_kernel,
        out_shape=pltpu.VMEM((columns, depth), jnp.bfloat16),
        cost_estimate=cost(columns, depth, rank),
        name="merge",
    )(weight, low_t, high)


def merge(me, weight, low_t, high, total):
    depth, columns = weight.shape
    rank = high.shape[0]
    block = next(b for b in (512, 256, 128) if columns % b == 0)
    if columns == block and block > 128:
        block //= 2
    return pl.pallas_call(
        merge_kernel,
        grid_spec=pltpu.PrefetchScalarGridSpec(
            num_scalar_prefetch=1,
            grid=(columns // block,),
            in_specs=[
                pl.BlockSpec((depth, block), lambda j, me: (0, j)),
                pl.BlockSpec((rank, depth), lambda j, me: (0, 0)),
                pl.BlockSpec((rank, block), lambda j, me: (0, j)),
            ],
            out_specs=[
                pl.BlockSpec((block, depth), lambda j, me: (j, 0)),
                pl.BlockSpec((block, depth), lambda j, me: (j, me[0])),
            ],
        ),
        out_shape=[
            jax.ShapeDtypeStruct((columns, depth), jnp.bfloat16),
            jax.ShapeDtypeStruct((columns, total), jnp.bfloat16),
        ],
        cost_estimate=cost(columns, depth, rank),
        name="merge",
    )(me, weight, low_t, high)


def source_of(me, r, parity):
    down = lax.rem(me + parity, 2) == 0
    return jnp.where(down, me + r, me - r)


def place_kernel(n, r, parity, pieces, me_ref, chunk_ref, *refs):
    staged = pieces > 1
    out_ref, sem, *stage = refs[-4:] if staged else refs[-2:]
    rows, depth = chunk_ref.shape
    step = rows // pieces
    source = me_ref[0] if r == 0 else source_of(me_ref[0], r, parity)

    @pl.when((source >= 0) & (source < n))
    def _():
        column = pl.multiple_of(source * depth, 128)
        parts = [pl.ds(p * step, step) for p in range(pieces)]
        held = stage[1] if staged else chunk_ref
        ins = [
            pltpu.make_async_copy(chunk_ref.at[part], held.at[part], stage[0].at[p])
            for p, part in enumerate(parts)
            if staged
        ]
        outs = [
            pltpu.make_async_copy(held.at[part], out_ref.at[part, pl.ds(column, depth)], sem.at[p])
            for p, part in enumerate(parts)
        ]
        for copy in ins:
            copy.start()
        for p in range(pieces):
            if staged:
                ins[p].wait()
            outs[p].start()
        for copy in outs:
            copy.wait()


def place(me, n, r, parity, chunk, out, in_vmem):
    rows, depth = chunk.shape
    pieces = 1 if in_vmem else 4
    sems = pltpu.SemaphoreType.DMA((pieces,))
    scratch, operands, aliases = [sems], [me, chunk], {}
    if in_vmem:
        operands[1] = pltpu.with_memory_space_constraint(chunk, pltpu.VMEM)
    else:
        scratch += [sems, pltpu.VMEM((rows, depth), jnp.bfloat16)]
    if isinstance(out, jax.Array):
        operands.append(out)
        aliases = {2: 0}
    specs = [pl.BlockSpec(memory_space=pltpu.VMEM if in_vmem else pl.ANY)]
    specs += [pl.BlockSpec(memory_space=pl.ANY)] * (len(operands) - 2)
    return pl.pallas_call(
        functools.partial(place_kernel, n, r, parity, pieces),
        grid_spec=pltpu.PrefetchScalarGridSpec(
            num_scalar_prefetch=1,
            grid=(1,),
            in_specs=specs,
            out_specs=pl.BlockSpec(memory_space=pl.ANY),
            scratch_shapes=scratch,
        ),
        out_shape=jax.ShapeDtypeStruct(out.shape, out.dtype),
        input_output_aliases=aliases,
        cost_estimate=pl.CostEstimate(
            flops=rows * depth, bytes_accessed=4 * rows * depth, transcendentals=0
        ),
        name="place",
    )(*operands)


def hop_pairs(n, r, parity):
    pairs = []
    for i in range(parity, n - 1, 2):
        if i - r + 1 >= 0:
            pairs.append((i, i + 1))
        if i + r <= n - 1:
            pairs.append((i + 1, i))
    return pairs


def steps_of(n):
    def hops(r, chunks, parities=(0, 1)):
        return [
            ("hop", r, parity, chunk)
            for parity in parities
            for chunk in chunks
            if hop_pairs(n, r, parity)
        ]

    steps = []
    for chunk in (FIRST, QUERY):
        steps.append(("merge", 0, 0, chunk))
        steps += hops(1, [chunk], [0])
    steps += hops(1, [FIRST, QUERY], [1])
    steps.append(("place", 0, 0, FIRST))
    steps.append(("merge", 0, 0, LAST))
    steps += hops(1, [LAST])
    steps.append(("exchange", 0, 0, NORM))
    steps += hops(1, [NORM])
    for r in range(2, n + 1):
        for chunk in CHUNKS:
            steps += hops(r, [chunk])
            if chunk is NORM:
                if r == n:
                    steps.append(("norm", 0, 0, NORM))
                continue
            for parity in (0, 1):
                if hop_pairs(n, r - 1, parity):
                    steps.append(("place", r - 1, parity, chunk))
    return steps


def gathered(arrays, norm_train, norm_step):
    serve = [
        lax.all_gather(
            (
                weight.astype(jnp.float32)
                + mix_rate * jnp.dot(low, high, preferred_element_type=jnp.float32)
            ).astype(jnp.bfloat16),
            "shard",
            axis=0,
            tiled=True,
        ).T
        for weight, low, high in arrays
    ]
    share = (norm_train + norm_step).astype(jnp.bfloat16)
    return (*serve, lax.all_gather(share, ("shard", "tp"), axis=0, tiled=True))


def solution(mesh):
    n, nt = mesh.shape["shard"], mesh.shape["tp"]
    steps = steps_of(n)

    def on_device(
        weight_query,
        low_query,
        high_query,
        weight_key,
        low_key,
        high_key,
        weight_value,
        low_value,
        high_value,
        norm_train,
        norm_step,
    ):
        depth = weight_query.shape[0]
        if depth % 128 or any(w.shape[1] % 128 for w in (weight_query, weight_key, weight_value)):
            arrays = (
                (weight_query, low_query, high_query),
                (weight_key, low_key, high_key),
                (weight_value, low_value, high_value),
            )
            return gathered(arrays, norm_train, norm_step)
        me = lax.axis_index("shard")
        me_ref = jnp.reshape(me, (1,)).astype(jnp.int32)
        mine = lax.axis_index("tp")
        inputs = {
            KEY: (weight_key, low_key.T, high_key),
            QUERY: (weight_query, low_query.T, high_query),
            VALUE: (weight_value, low_value.T, high_value),
        }
        outs = {}
        got = {}
        for what, r, parity, chunk in steps:
            if what == "merge":
                if chunk == FIRST:
                    piece = merge_first(*inputs[chunk])
                    outs[chunk] = jax.ShapeDtypeStruct((piece.shape[0], depth * n), piece.dtype)
                else:
                    piece, outs[chunk] = merge(me_ref, *inputs[chunk], depth * n)
                got[0, 0, chunk] = got[0, 1, chunk] = piece
            elif what == "exchange":
                share = (norm_train + norm_step).astype(jnp.bfloat16)
                shares = [share] + [
                    lax.ppermute(share, "tp", [(j, (j + k) % nt) for j in range(nt)])
                    for k in range(1, nt)
                ]
                parts = []
                for j in range(nt):
                    part = share
                    for k in range(1, nt):
                        part = jnp.where(mine == (j + k) % nt, shares[k], part)
                    parts.append(part)
                got[0, 0, NORM] = got[0, 1, NORM] = jnp.concatenate(parts)
            elif what == "hop":
                held = got[r - 1, 1 - parity, chunk]
                got[r, parity, chunk] = lax.ppermute(held, "shard", hop_pairs(n, r, parity))
            elif what == "place":
                in_vmem = r == 0 or (r == n - 1 and chunk == LAST)
                outs[chunk] = place(me_ref, n, r, parity, got[r, parity, chunk], outs[chunk], in_vmem)
            else:
                rows = []
                for s in range(n):
                    row = got[0, 0, NORM]
                    for (r, parity, chunk), value in got.items():
                        if chunk is NORM and r > 0:
                            row = jnp.where(source_of(me, r, parity) == s, value, row)
                    rows.append(row)
                serve_norm = jnp.concatenate(rows)
        return outs[QUERY], outs[KEY], outs[VALUE], serve_norm

    in_specs = (
        P(("trial", "shard"), "tp"),
        P(("trial", "shard"), None),
        P("trial", "tp"),
        P(("trial", "shard"), "tp"),
        P(("trial", "shard"), None),
        P("trial", "tp"),
        P(("trial", "shard"), "tp"),
        P(("trial", "shard"), None),
        P("trial", "tp"),
        P(("trial", "shard", "tp")),
        P(("trial", "shard", "tp")),
    )
    out_specs = (
        P(("trial", "tp"), None),
        P(("trial", "tp"), None),
        P(("trial", "tp"), None),
        P("trial"),
    )
    return jax.shard_map(
        on_device, mesh=mesh, in_specs=in_specs, out_specs=out_specs, check_vma=False
    )
```

```python
import functools

import jax
import jax.numpy as jnp
from jax import lax
from jax.experimental import pallas as pl
from jax.experimental.pallas import tpu as pltpu
from jax.sharding import PartitionSpec as P

mix_rate = 1.0


KEY, QUERY, VALUE = range(3)
EIGHTHS = 8
FIRST, KEY_REST = (KEY, 0, 4), (KEY, 4, 4)
QUERY_ALL = (QUERY, 0, 8)
NORM = None
VALUE_REST, LAST = (VALUE, 0, 6), (VALUE, 6, 2)
CHUNKS = (FIRST, KEY_REST, QUERY_ALL, NORM, VALUE_REST, LAST)


def extent(columns, chunk):
    return columns * chunk[1] // EIGHTHS, columns * chunk[2] // EIGHTHS


def merged(weight_ref, low_ref, high_ref):
    delta = lax.dot_general(
        high_ref[...], low_ref[...], (((0,), (0,)), ((), ())), preferred_element_type=jnp.float32
    )
    fresh = weight_ref[...].T.astype(jnp.float32) + mix_rate * delta
    return fresh.astype(jnp.bfloat16)


def first_kernel(weight_ref, low_ref, high_ref, chunk_ref):
    chunk_ref[...] = merged(weight_ref, low_ref, high_ref)


def merge_kernel(me_ref, weight_ref, low_ref, high_ref, *refs):
    chunk_ref, out_ref = refs[-2:]
    fresh = merged(weight_ref, low_ref, high_ref)
    chunk_ref[...] = fresh
    out_ref[...] = fresh


def cost(rows, depth, rank):
    return pl.CostEstimate(
        flops=2 * rows * depth * rank, bytes_accessed=6 * rows * depth, transcendentals=0
    )


def merge_first(weight, low_t, high, chunk):
    depth, columns = weight.shape
    rank = high.shape[0]
    start, rows = extent(columns, chunk)
    first = start // rows
    return pl.pallas_call(
        first_kernel,
        grid=(1,),
        in_specs=[
            pl.BlockSpec((depth, rows), lambda j: (0, first)),
            pl.BlockSpec((rank, depth), lambda j: (0, 0)),
            pl.BlockSpec((rank, rows), lambda j: (0, first)),
        ],
        out_specs=pl.BlockSpec(memory_space=pltpu.VMEM),
        out_shape=pltpu.VMEM((rows, depth), jnp.bfloat16),
        cost_estimate=cost(rows, depth, rank),
        name="merge",
    )(weight, low_t, high)


def merge(me, weight, low_t, high, chunk, out):
    depth, columns = weight.shape
    rank = high.shape[0]
    start, rows = extent(columns, chunk)
    block = next(b for b in (512, 384, 256, 128) if start % b == 0 and rows % b == 0)
    first = start // block
    specs = [
        pl.BlockSpec((depth, block), lambda j, me: (0, first + j)),
        pl.BlockSpec((rank, depth), lambda j, me: (0, 0)),
        pl.BlockSpec((rank, block), lambda j, me: (0, first + j)),
    ]
    operands, aliases = [me, weight, low_t, high], {}
    if isinstance(out, jax.Array):
        specs.append(pl.BlockSpec(memory_space=pl.ANY))
        operands.append(out)
        aliases = {4: 1}
    return pl.pallas_call(
        merge_kernel,
        grid_spec=pltpu.PrefetchScalarGridSpec(
            num_scalar_prefetch=1,
            grid=(rows // block,),
            in_specs=specs,
            out_specs=[
                pl.BlockSpec((block, depth), lambda j, me: (j, 0)),
                pl.BlockSpec((block, depth), lambda j, me: (first + j, me[0])),
            ],
        ),
        out_shape=[
            jax.ShapeDtypeStruct((rows, depth), jnp.bfloat16),
            jax.ShapeDtypeStruct(out.shape, jnp.bfloat16),
        ],
        input_output_aliases=aliases,
        cost_estimate=cost(rows, depth, rank),
        name="merge",
    )(*operands)


def source_of(me, r, parity):
    down = lax.rem(me + parity, 2) == 0
    return jnp.where(down, me + r, me - r)


def place_kernel(n, r, parity, start, me_ref, chunk_ref, _, out_ref, sem, stage=None):
    rows, depth = chunk_ref.shape
    source = me_ref[0] if r == 0 else source_of(me_ref[0], r, parity)

    @pl.when((source >= 0) & (source < n))
    def _():
        held = chunk_ref
        if stage is not None:
            held = stage
            copy = pltpu.make_async_copy(chunk_ref, held, sem.at[1])
            copy.start()
            copy.wait()
        column = pl.multiple_of(source * depth, 128)
        there = out_ref.at[pl.ds(start, rows), pl.ds(column, depth)]
        copy = pltpu.make_async_copy(held, there, sem.at[0])
        copy.start()
        copy.wait()


def place(me, n, r, parity, chunk, out, start, in_vmem):
    rows, depth = chunk.shape
    scratch = [pltpu.SemaphoreType.DMA((2,))]
    if in_vmem:
        chunk = pltpu.with_memory_space_constraint(chunk, pltpu.VMEM)
    else:
        scratch.append(pltpu.VMEM((rows, depth), jnp.bfloat16))
    return pl.pallas_call(
        functools.partial(place_kernel, n, r, parity, start),
        grid_spec=pltpu.PrefetchScalarGridSpec(
            num_scalar_prefetch=1,
            grid=(1,),
            in_specs=[
                pl.BlockSpec(memory_space=pltpu.VMEM if in_vmem else pl.ANY),
                pl.BlockSpec(memory_space=pl.ANY),
            ],
            out_specs=pl.BlockSpec(memory_space=pl.ANY),
            scratch_shapes=scratch,
        ),
        out_shape=jax.ShapeDtypeStruct(out.shape, out.dtype),
        input_output_aliases={2: 0},
        cost_estimate=pl.CostEstimate(
            flops=rows * depth, bytes_accessed=4 * rows * depth, transcendentals=0
        ),
        name="place",
    )(me, chunk, out)


def hop_pairs(n, r, parity):
    pairs = []
    for i in range(parity, n - 1, 2):
        if i - r + 1 >= 0:
            pairs.append((i, i + 1))
        if i + r <= n - 1:
            pairs.append((i + 1, i))
    return pairs


def steps_of(n):
    def hops(r, chunks, parities=(0, 1)):
        return [
            ("hop", r, parity, chunk)
            for parity in parities
            for chunk in chunks
            if hop_pairs(n, r, parity)
        ]

    steps = []
    early, late = (FIRST, KEY_REST, QUERY_ALL), (VALUE_REST, LAST)
    for chunk in early:
        steps.append(("merge", 0, 0, chunk))
        steps += hops(1, [chunk], [0])
    steps += hops(1, early, [1])
    steps.append(("place", 0, 0, FIRST))
    steps += [("merge", 0, 0, chunk) for chunk in late]
    steps += hops(1, late)
    steps.append(("exchange", 0, 0, NORM))
    steps += hops(1, [NORM])
    for r in range(2, n + 1):
        for chunk in CHUNKS:
            steps += hops(r, [chunk])
            if chunk is NORM:
                if r == n:
                    steps.append(("norm", 0, 0, NORM))
                continue
            for parity in (0, 1):
                if hop_pairs(n, r - 1, parity):
                    steps.append(("place", r - 1, parity, chunk))
    return steps


def gathered(arrays, norm_train, norm_step):
    serve = [
        lax.all_gather(
            (
                weight.astype(jnp.float32)
                + mix_rate * jnp.dot(low, high, preferred_element_type=jnp.float32)
            ).astype(jnp.bfloat16),
            "shard",
            axis=0,
            tiled=True,
        ).T
        for weight, low, high in arrays
    ]
    share = (norm_train + norm_step).astype(jnp.bfloat16)
    return (*serve, lax.all_gather(share, ("shard", "tp"), axis=0, tiled=True))


def solution(mesh):
    n, nt = mesh.shape["shard"], mesh.shape["tp"]
    steps = steps_of(n)

    def on_device(
        weight_query,
        low_query,
        high_query,
        weight_key,
        low_key,
        high_key,
        weight_value,
        low_value,
        high_value,
        norm_train,
        norm_step,
    ):
        depth = weight_query.shape[0]
        if depth % 128 or any(w.shape[1] % 512 for w in (weight_query, weight_key, weight_value)):
            arrays = (
                (weight_query, low_query, high_query),
                (weight_key, low_key, high_key),
                (weight_value, low_value, high_value),
            )
            return gathered(arrays, norm_train, norm_step)
        me = lax.axis_index("shard")
        me_ref = jnp.reshape(me, (1,)).astype(jnp.int32)
        mine = lax.axis_index("tp")
        inputs = {
            KEY: (weight_key, low_key.T, high_key),
            QUERY: (weight_query, low_query.T, high_query),
            VALUE: (weight_value, low_value.T, high_value),
        }
        outs = {}
        got = {}
        for what, r, parity, chunk in steps:
            if what == "merge":
                weight, low_t, high = inputs[chunk[0]]
                if chunk == FIRST:
                    piece = merge_first(weight, low_t, high, chunk)
                else:
                    shape = jax.ShapeDtypeStruct((weight.shape[1], depth * n), jnp.bfloat16)
                    out = outs.get(chunk[0], shape)
                    piece, outs[chunk[0]] = merge(me_ref, weight, low_t, high, chunk, out)
                got[0, 0, chunk] = got[0, 1, chunk] = piece
            elif what == "exchange":
                share = (norm_train + norm_step).astype(jnp.bfloat16)
                shares = [share] + [
                    lax.ppermute(share, "tp", [(j, (j + k) % nt) for j in range(nt)])
                    for k in range(1, nt)
                ]
                parts = []
                for j in range(nt):
                    part = share
                    for k in range(1, nt):
                        part = jnp.where(mine == (j + k) % nt, shares[k], part)
                    parts.append(part)
                got[0, 0, NORM] = got[0, 1, NORM] = jnp.concatenate(parts)
            elif what == "hop":
                held = got[r - 1, 1 - parity, chunk]
                got[r, parity, chunk] = lax.ppermute(held, "shard", hop_pairs(n, r, parity))
            elif what == "place":
                piece, out = got[r, parity, chunk], outs[chunk[0]]
                start, _ = extent(out.shape[0], chunk)
                in_vmem = r == 0 or (r == n - 1 and chunk[0] == VALUE)
                outs[chunk[0]] = place(me_ref, n, r, parity, piece, out, start, in_vmem)
            else:
                rows = []
                for s in range(n):
                    row = got[0, 0, NORM]
                    for (r, parity, chunk), value in got.items():
                        if chunk is NORM and r > 0:
                            row = jnp.where(source_of(me, r, parity) == s, value, row)
                    rows.append(row)
                serve_norm = jnp.concatenate(rows)
        return outs[QUERY], outs[KEY], outs[VALUE], serve_norm

    in_specs = (
        P(("trial", "shard"), "tp"),
        P(("trial", "shard"), None),
        P("trial", "tp"),
        P(("trial", "shard"), "tp"),
        P(("trial", "shard"), None),
        P("trial", "tp"),
        P(("trial", "shard"), "tp"),
        P(("trial", "shard"), None),
        P("trial", "tp"),
        P(("trial", "shard", "tp")),
        P(("trial", "shard", "tp")),
    )
    out_specs = (
        P(("trial", "tp"), None),
        P(("trial", "tp"), None),
        P(("trial", "tp"), None),
        P("trial"),
    )
    return jax.shard_map(
        on_device, mesh=mesh, in_specs=in_specs, out_specs=out_specs, check_vma=False
    )
```

```python
import functools

import jax
import jax.numpy as jnp
from jax import lax
from jax.experimental import pallas as pl
from jax.experimental.pallas import tpu as pltpu
from jax.sharding import PartitionSpec as P

mix_rate = 1.0


KEY, QUERY, VALUE = range(3)
FIRST, LAST, NORM = KEY, VALUE, None


def merged(weight_ref, low_ref, high_ref):
    delta = lax.dot_general(
        high_ref[...], low_ref[...], (((0,), (0,)), ((), ())), preferred_element_type=jnp.float32
    )
    fresh = weight_ref[...].T.astype(jnp.float32) + mix_rate * delta
    return fresh.astype(jnp.bfloat16)


def first_kernel(weight_ref, low_ref, high_ref, chunk_ref):
    chunk_ref[...] = merged(weight_ref, low_ref, high_ref)


def merge_kernel(me_ref, weight_ref, low_ref, high_ref, chunk_ref, out_ref):
    fresh = merged(weight_ref, low_ref, high_ref)
    chunk_ref[...] = fresh
    out_ref[...] = fresh


def cost(rows, depth, rank):
    return pl.CostEstimate(
        flops=2 * rows * depth * rank, bytes_accessed=6 * rows * depth, transcendentals=0
    )


def merge_first(weight, low_t, high):
    depth, columns = weight.shape
    rank = high.shape[0]
    return pl.pallas_call(
        first_kernel,
        out_shape=pltpu.VMEM((columns, depth), jnp.bfloat16),
        cost_estimate=cost(columns, depth, rank),
        name="merge",
    )(weight, low_t, high)


def merge(me, weight, low_t, high, total):
    depth, columns = weight.shape
    rank = high.shape[0]
    block = next(b for b in (512, 256, 128) if columns % b == 0)
    if columns == block and block > 128:
        block //= 2
    return pl.pallas_call(
        merge_kernel,
        grid_spec=pltpu.PrefetchScalarGridSpec(
            num_scalar_prefetch=1,
            grid=(columns // block,),
            in_specs=[
                pl.BlockSpec((depth, block), lambda j, me: (0, j)),
                pl.BlockSpec((rank, depth), lambda j, me: (0, 0)),
                pl.BlockSpec((rank, block), lambda j, me: (0, j)),
            ],
            out_specs=[
                pl.BlockSpec((block, depth), lambda j, me: (j, 0)),
                pl.BlockSpec((block, depth), lambda j, me: (j, me[0])),
            ],
        ),
        out_shape=[
            jax.ShapeDtypeStruct((columns, depth), jnp.bfloat16),
            jax.ShapeDtypeStruct((columns, total), jnp.bfloat16),
        ],
        cost_estimate=cost(columns, depth, rank),
        name="merge",
    )(me, weight, low_t, high)


def source_of(me, r, parity):
    down = lax.rem(me + parity, 2) == 0
    return jnp.where(down, me + r, me - r)


def place_kernel(n, hops, staged, me_ref, *refs):
    chunk_refs, refs = refs[: len(hops)], refs[-3:] if staged else (*refs[-2:], None)
    out_ref, sem, stage = refs

    for (r, parity), chunk_ref in zip(hops, chunk_refs):
        source = me_ref[0] if r == 0 else source_of(me_ref[0], r, parity)

        @pl.when((source >= 0) & (source < n))
        def _():
            held = chunk_ref
            if staged:
                held = stage
                copy = pltpu.make_async_copy(chunk_ref, held, sem.at[1])
                copy.start()
                copy.wait()
            depth = chunk_ref.shape[1]
            there = out_ref.at[:, pl.ds(pl.multiple_of(source * depth, 128), depth)]
            copy = pltpu.make_async_copy(held, there, sem.at[0])
            copy.start()
            copy.wait()


def place(me, n, hops, chunks, out, staged):
    rows, depth = chunks[0].shape
    scratch = [pltpu.SemaphoreType.DMA((2,))]
    specs = [pl.BlockSpec(memory_space=pl.ANY if staged else pltpu.VMEM)] * len(hops)
    if staged:
        scratch.append(pltpu.VMEM((rows, depth), jnp.bfloat16))
    else:
        chunks = [pltpu.with_memory_space_constraint(chunk, pltpu.VMEM) for chunk in chunks]
    operands, aliases = [me, *chunks], {}
    if isinstance(out, jax.Array):
        aliases = {len(operands): 0}
        operands.append(out)
        specs.append(pl.BlockSpec(memory_space=pl.ANY))
    return pl.pallas_call(
        functools.partial(place_kernel, n, hops, staged),
        grid_spec=pltpu.PrefetchScalarGridSpec(
            num_scalar_prefetch=1,
            grid=(1,),
            in_specs=specs,
            out_specs=pl.BlockSpec(memory_space=pl.ANY),
            scratch_shapes=scratch,
        ),
        out_shape=jax.ShapeDtypeStruct(out.shape, out.dtype),
        input_output_aliases=aliases,
        cost_estimate=pl.CostEstimate(
            flops=rows * depth, bytes_accessed=4 * rows * depth, transcendentals=0
        ),
        name="place",
    )(*operands)


def hop_pairs(n, r, parity):
    pairs = []
    for i in range(parity, n - 1, 2):
        if i - r + 1 >= 0:
            pairs.append((i, i + 1))
        if i + r <= n - 1:
            pairs.append((i + 1, i))
    return pairs


def steps_of(n):
    def hops(chunk, *pairs):
        return [("hop", pair, chunk) for pair in pairs if hop_pairs(n, *pair)]

    steps = []
    for chunk in (FIRST, QUERY):
        steps.append(("merge", None, chunk))
        steps += hops(chunk, (1, 0))
    steps += hops(FIRST, (1, 1)) + hops(QUERY, (1, 1))
    steps.append(("place", ((0, 0),), FIRST))
    steps.append(("merge", None, LAST))
    steps += hops(LAST, (1, 0), (1, 1))
    steps.append(("exchange", None, NORM))
    steps += [("shift", k, NORM) for k in range(1, n)]
    for r in range(2, n + 2):
        for chunk in (FIRST, QUERY, LAST):
            if r == n and chunk == LAST:
                steps.append(("norm", None, NORM))
            steps += hops(chunk, (r, 0), (r, 1))
            came = tuple(pair for pair in ((r - 1, 0), (r - 2, 1)) if r > 2 or pair[1] == 0)
            came = tuple(pair for pair in came if hop_pairs(n, *pair))
            if came:
                steps.append(("place", came, chunk))
    if n == 1:
        steps.append(("norm", None, NORM))
    return steps


def ordered(shifted, me, n):
    parts = []
    for j in range(n):
        part = shifted[0]
        for k in range(1, n):
            part = jnp.where(me == (j + k) % n, shifted[k], part)
        parts.append(part)
    return parts


def gathered(arrays, norm_train, norm_step):
    serve = [
        lax.all_gather(
            (
                weight.astype(jnp.float32)
                + mix_rate * jnp.dot(low, high, preferred_element_type=jnp.float32)
            ).astype(jnp.bfloat16),
            "shard",
            axis=0,
            tiled=True,
        ).T
        for weight, low, high in arrays
    ]
    share = (norm_train + norm_step).astype(jnp.bfloat16)
    return (*serve, lax.all_gather(share, ("shard", "tp"), axis=0, tiled=True))


def solution(mesh):
    n, nt = mesh.shape["shard"], mesh.shape["tp"]
    steps = steps_of(n)

    def on_device(
        weight_query,
        low_query,
        high_query,
        weight_key,
        low_key,
        high_key,
        weight_value,
        low_value,
        high_value,
        norm_train,
        norm_step,
    ):
        depth = weight_query.shape[0]
        if depth % 128 or any(w.shape[1] % 128 for w in (weight_query, weight_key, weight_value)):
            arrays = (
                (weight_query, low_query, high_query),
                (weight_key, low_key, high_key),
                (weight_value, low_value, high_value),
            )
            return gathered(arrays, norm_train, norm_step)
        me = lax.axis_index("shard")
        me_ref = jnp.reshape(me, (1,)).astype(jnp.int32)
        mine = lax.axis_index("tp")
        inputs = {
            KEY: (weight_key, low_key.T, high_key),
            QUERY: (weight_query, low_query.T, high_query),
            VALUE: (weight_value, low_value.T, high_value),
        }
        outs = {}
        got = {}
        for what, hop, chunk in steps:
            if what == "merge":
                if chunk == FIRST:
                    piece = merge_first(*inputs[chunk])
                    outs[chunk] = jax.ShapeDtypeStruct((piece.shape[0], depth * n), piece.dtype)
                else:
                    piece, outs[chunk] = merge(me_ref, *inputs[chunk], depth * n)
                got[(0, 0), chunk] = got[(0, 1), chunk] = piece
            elif what == "hop":
                r, parity = hop
                held = got[(r - 1, 1 - parity), chunk]
                got[hop, chunk] = lax.ppermute(held, "shard", hop_pairs(n, r, parity))
            elif what == "place":
                pieces = [got[pair, chunk] for pair in hop]
                staged = not (hop[0][0] == 0 or (hop[0][0] >= n - 1 and chunk == LAST))
                outs[chunk] = place(me_ref, n, hop, pieces, outs[chunk], staged)
            elif what == "exchange":
                share = (norm_train + norm_step).astype(jnp.bfloat16)
                shares = [share] + [
                    lax.ppermute(share, "tp", [(j, (j + k) % nt) for j in range(nt)])
                    for k in range(1, nt)
                ]
                rows = [jnp.concatenate(ordered(shares, mine, nt))]
            elif what == "shift":
                rows.append(lax.ppermute(rows[0], "shard", [(j, (j + hop) % n) for j in range(n)]))
            else:
                serve_norm = jnp.concatenate(ordered(rows, me, n))
        return outs[QUERY], outs[KEY], outs[VALUE], serve_norm

    in_specs = (
        P(("trial", "shard"), "tp"),
        P(("trial", "shard"), None),
        P("trial", "tp"),
        P(("trial", "shard"), "tp"),
        P(("trial", "shard"), None),
        P("trial", "tp"),
        P(("trial", "shard"), "tp"),
        P(("trial", "shard"), None),
        P("trial", "tp"),
        P(("trial", "shard", "tp")),
        P(("trial", "shard", "tp")),
    )
    out_specs = (
        P(("trial", "tp"), None),
        P(("trial", "tp"), None),
        P(("trial", "tp"), None),
        P("trial"),
    )
    return jax.shard_map(
        on_device, mesh=mesh, in_specs=in_specs, out_specs=out_specs, check_vma=False
    )
```

```python
import functools

import jax
import jax.numpy as jnp
from jax import lax
from jax.experimental import pallas as pl
from jax.experimental.pallas import tpu as pltpu
from jax.sharding import PartitionSpec as P

mix_rate = 1.0


KEY, QUERY, VALUE = range(3)
FIRST, LAST, NORM = KEY, VALUE, None
LEAD, REST = "lead", "rest"


def merged(weight_ref, low_ref, high_ref):
    delta = lax.dot_general(
        high_ref[...], low_ref[...], (((0,), (0,)), ((), ())), preferred_element_type=jnp.float32
    )
    fresh = weight_ref[...].T.astype(jnp.float32) + mix_rate * delta
    return fresh.astype(jnp.bfloat16)


def first_kernel(start, weight_ref, low_ref, high_ref, chunk_ref, weight, low, high, sem):
    columns = pl.ds(start, chunk_ref.shape[0])
    copies = [
        pltpu.make_async_copy(weight_ref.at[:, columns], weight, sem.at[0]),
        pltpu.make_async_copy(low_ref, low, sem.at[1]),
        pltpu.make_async_copy(high_ref.at[:, columns], high, sem.at[2]),
    ]
    for copy in copies:
        copy.start()
    for copy in copies:
        copy.wait()
    chunk_ref[...] = merged(weight, low, high)


def merge_kernel(me_ref, weight_ref, low_ref, high_ref, chunk_ref, out_ref):
    fresh = merged(weight_ref, low_ref, high_ref)
    chunk_ref[...] = fresh
    out_ref[...] = fresh


def cost(rows, depth, rank):
    return pl.CostEstimate(
        flops=2 * rows * depth * rank, bytes_accessed=6 * rows * depth, transcendentals=0
    )


def merge_first(weight, low_t, high, start, rows):
    depth, rank = weight.shape[0], high.shape[0]
    return pl.pallas_call(
        functools.partial(first_kernel, start),
        in_specs=[pl.BlockSpec(memory_space=pl.ANY)] * 3,
        out_specs=pl.BlockSpec(memory_space=pltpu.VMEM),
        out_shape=pltpu.VMEM((rows, depth), jnp.bfloat16),
        scratch_shapes=[
            pltpu.VMEM((depth, rows), jnp.bfloat16),
            pltpu.VMEM((rank, depth), jnp.bfloat16),
            pltpu.VMEM((rank, rows), jnp.bfloat16),
            pltpu.SemaphoreType.DMA((3,)),
        ],
        cost_estimate=cost(rows, depth, rank),
        name="merge",
    )(weight, low_t, high)


def merge(me, weight, low_t, high, total):
    depth, columns = weight.shape
    rank = high.shape[0]
    block = next(b for b in (512, 256, 128) if columns % (2 * b) == 0)
    return pl.pallas_call(
        merge_kernel,
        grid_spec=pltpu.PrefetchScalarGridSpec(
            num_scalar_prefetch=1,
            grid=(columns // block,),
            in_specs=[
                pl.BlockSpec((depth, block), lambda j, me: (0, j)),
                pl.BlockSpec((rank, depth), lambda j, me: (0, 0)),
                pl.BlockSpec((rank, block), lambda j, me: (0, j)),
            ],
            out_specs=[
                pl.BlockSpec((block, depth), lambda j, me: (j, 0)),
                pl.BlockSpec((block, depth), lambda j, me: (j, me[0])),
            ],
        ),
        out_shape=[
            jax.ShapeDtypeStruct((columns, depth), jnp.bfloat16),
            jax.ShapeDtypeStruct((columns, total), jnp.bfloat16),
        ],
        cost_estimate=cost(columns, depth, rank),
        name="merge",
    )(me, weight, low_t, high)


def source_of(me, r, parity):
    down = lax.rem(me + parity, 2) == 0
    return jnp.where(down, me + r, me - r)


def place_kernel(n, hops, staged, me_ref, *refs):
    chunk_refs, refs = refs[: len(hops)], refs[-3:] if staged else (*refs[-2:], None)
    out_ref, sem, stage = refs

    for (r, parity), chunk_ref in zip(hops, chunk_refs):
        source = me_ref[0] if r == 0 else source_of(me_ref[0], r, parity)

        @pl.when((source >= 0) & (source < n))
        def _():
            held = chunk_ref
            if staged:
                held = stage
                copy = pltpu.make_async_copy(chunk_ref, held, sem.at[1])
                copy.start()
                copy.wait()
            depth = chunk_ref.shape[1]
            there = out_ref.at[:, pl.ds(pl.multiple_of(source * depth, 128), depth)]
            copy = pltpu.make_async_copy(held, there, sem.at[0])
            copy.start()
            copy.wait()


def place(me, n, hops, chunks, out, staged):
    rows, depth = chunks[0].shape
    scratch = [pltpu.SemaphoreType.DMA((2,))]
    specs = [pl.BlockSpec(memory_space=pl.ANY if staged else pltpu.VMEM)] * len(hops)
    if staged:
        scratch.append(pltpu.VMEM((rows, depth), jnp.bfloat16))
    else:
        chunks = [pltpu.with_memory_space_constraint(chunk, pltpu.VMEM) for chunk in chunks]
    operands, aliases = [me, *chunks], {}
    if isinstance(out, jax.Array):
        aliases = {len(operands): 0}
        operands.append(out)
        specs.append(pl.BlockSpec(memory_space=pl.ANY))
    return pl.pallas_call(
        functools.partial(place_kernel, n, hops, staged),
        grid_spec=pltpu.PrefetchScalarGridSpec(
            num_scalar_prefetch=1,
            grid=(1,),
            in_specs=specs,
            out_specs=pl.BlockSpec(memory_space=pl.ANY),
            scratch_shapes=scratch,
        ),
        out_shape=jax.ShapeDtypeStruct(out.shape, out.dtype),
        input_output_aliases=aliases,
        cost_estimate=pl.CostEstimate(
            flops=rows * depth, bytes_accessed=4 * rows * depth, transcendentals=0
        ),
        name="place",
    )(*operands)


def hop_pairs(n, r, parity):
    pairs = []
    for i in range(parity, n - 1, 2):
        if i - r + 1 >= 0:
            pairs.append((i, i + 1))
        if i + r <= n - 1:
            pairs.append((i + 1, i))
    return pairs


def steps_of(n):
    def hops(chunk, *pairs):
        return [("hop", pair, chunk) for pair in pairs if hop_pairs(n, *pair)]

    steps = []
    for chunk in (LEAD, REST, QUERY):
        steps.append(("merge", None, chunk))
        steps += hops(chunk, (1, 0))
    steps.append(("join", None, FIRST))
    steps += hops(FIRST, (1, 1)) + hops(QUERY, (1, 1))
    steps.append(("place", ((0, 0),), FIRST))
    steps.append(("merge", None, LAST))
    steps += hops(LAST, (1, 0), (1, 1))
    steps.append(("exchange", None, NORM))
    steps += [("shift", k, NORM) for k in range(1, n)]
    for r in range(2, n + 2):
        for chunk in (FIRST, QUERY, LAST):
            if r == n and chunk == LAST:
                steps.append(("norm", None, NORM))
            steps += hops(chunk, (r, 0), (r, 1))
            came = tuple(pair for pair in ((r - 1, 0), (r - 2, 1)) if r > 2 or pair[1] == 0)
            came = tuple(pair for pair in came if hop_pairs(n, *pair))
            if came:
                steps.append(("place", came, chunk))
    if n == 1:
        steps.append(("norm", None, NORM))
    return steps


def ordered(shifted, me, n):
    parts = []
    for j in range(n):
        part = shifted[0]
        for k in range(1, n):
            part = jnp.where(me == (j + k) % n, shifted[k], part)
        parts.append(part)
    return parts


def gathered(arrays, norm_train, norm_step):
    serve = [
        lax.all_gather(
            (
                weight.astype(jnp.float32)
                + mix_rate * jnp.dot(low, high, preferred_element_type=jnp.float32)
            ).astype(jnp.bfloat16),
            "shard",
            axis=0,
            tiled=True,
        ).T
        for weight, low, high in arrays
    ]
    share = (norm_train + norm_step).astype(jnp.bfloat16)
    return (*serve, lax.all_gather(share, ("shard", "tp"), axis=0, tiled=True))


def solution(mesh):
    n, nt = mesh.shape["shard"], mesh.shape["tp"]
    steps = steps_of(n)

    def on_device(
        weight_query,
        low_query,
        high_query,
        weight_key,
        low_key,
        high_key,
        weight_value,
        low_value,
        high_value,
        norm_train,
        norm_step,
    ):
        depth = weight_query.shape[0]
        if depth % 128 or any(w.shape[1] % 256 for w in (weight_query, weight_key, weight_value)):
            arrays = (
                (weight_query, low_query, high_query),
                (weight_key, low_key, high_key),
                (weight_value, low_value, high_value),
            )
            return gathered(arrays, norm_train, norm_step)
        me = lax.axis_index("shard")
        me_ref = jnp.reshape(me, (1,)).astype(jnp.int32)
        mine = lax.axis_index("tp")
        inputs = {
            KEY: (weight_key, low_key.T, high_key),
            QUERY: (weight_query, low_query.T, high_query),
            VALUE: (weight_value, low_value.T, high_value),
        }
        outs = {}
        got = {}
        for what, hop, chunk in steps:
            if what == "merge":
                if chunk in (LEAD, REST):
                    rows = inputs[FIRST][0].shape[1]
                    lead = rows // 2
                    part = (0, lead) if chunk == LEAD else (lead, rows - lead)
                    piece = merge_first(*inputs[FIRST], *part)
                    outs[FIRST] = jax.ShapeDtypeStruct((rows, depth * n), piece.dtype)
                else:
                    piece, outs[chunk] = merge(me_ref, *inputs[chunk], depth * n)
                got[(0, 0), chunk] = got[(0, 1), chunk] = piece
            elif what == "join":
                for pair in ((0, 0), (0, 1), (1, 0)):
                    if (pair, LEAD) in got:
                        parts = [got[pair, LEAD], got[pair, REST]]
                        got[pair, FIRST] = jnp.concatenate(parts)
            elif what == "hop":
                r, parity = hop
                held = got[(r - 1, 1 - parity), chunk]
                got[hop, chunk] = lax.ppermute(held, "shard", hop_pairs(n, r, parity))
            elif what == "place":
                pieces = [got[pair, chunk] for pair in hop]
                staged = not (hop[0][0] == 0 or (hop[0][0] >= n - 1 and chunk == LAST))
                outs[chunk] = place(me_ref, n, hop, pieces, outs[chunk], staged)
            elif what == "exchange":
                share = (norm_train + norm_step).astype(jnp.bfloat16)
                shares = [share] + [
                    lax.ppermute(share, "tp", [(j, (j + k) % nt) for j in range(nt)])
                    for k in range(1, nt)
                ]
                rows = [jnp.concatenate(ordered(shares, mine, nt))]
            elif what == "shift":
                rows.append(lax.ppermute(rows[0], "shard", [(j, (j + hop) % n) for j in range(n)]))
            else:
                serve_norm = jnp.concatenate(ordered(rows, me, n))
        return outs[QUERY], outs[KEY], outs[VALUE], serve_norm

    in_specs = (
        P(("trial", "shard"), "tp"),
        P(("trial", "shard"), None),
        P("trial", "tp"),
        P(("trial", "shard"), "tp"),
        P(("trial", "shard"), None),
        P("trial", "tp"),
        P(("trial", "shard"), "tp"),
        P(("trial", "shard"), None),
        P("trial", "tp"),
        P(("trial", "shard", "tp")),
        P(("trial", "shard", "tp")),
    )
    out_specs = (
        P(("trial", "tp"), None),
        P(("trial", "tp"), None),
        P(("trial", "tp"), None),
        P("trial"),
    )
    return jax.shard_map(
        on_device, mesh=mesh, in_specs=in_specs, out_specs=out_specs, check_vma=False
    )
```

```python
import functools

import jax
import jax.numpy as jnp
from jax import lax
from jax.experimental import pallas as pl
from jax.experimental.pallas import tpu as pltpu
from jax.sharding import PartitionSpec as P

mix_rate = 1.0


KEY, QUERY, VALUE = range(3)
FIRST, LAST, NORM = KEY, VALUE, None


def merged(weight_ref, low_ref, high_ref):
    delta = lax.dot_general(
        high_ref[...], low_ref[...], (((0,), (0,)), ((), ())), preferred_element_type=jnp.float32
    )
    fresh = weight_ref[...].T.astype(jnp.float32) + mix_rate * delta
    return fresh.astype(jnp.bfloat16)


def first_kernel(weight_ref, low_ref, high_ref, chunk_ref):
    chunk_ref[...] = merged(weight_ref, low_ref, high_ref)


def merge_kernel(me_ref, weight_ref, low_ref, high_ref, chunk_ref, out_ref):
    fresh = merged(weight_ref, low_ref, high_ref)
    chunk_ref[...] = fresh
    out_ref[...] = fresh


def cost(rows, depth, rank):
    return pl.CostEstimate(
        flops=2 * rows * depth * rank, bytes_accessed=6 * rows * depth, transcendentals=0
    )


def merge_first(weight, low_t, high):
    depth, columns = weight.shape
    rank = high.shape[0]
    return pl.pallas_call(
        first_kernel,
        out_shape=pltpu.VMEM((columns, depth), jnp.bfloat16),
        cost_estimate=cost(columns, depth, rank),
        name="merge",
    )(weight, low_t, high)


def merge(me, weight, low_t, high, total):
    depth, columns = weight.shape
    rank = high.shape[0]
    block = next(b for b in (512, 256, 128) if columns % b == 0)
    if columns == block and block > 128:
        block //= 2
    return pl.pallas_call(
        merge_kernel,
        grid_spec=pltpu.PrefetchScalarGridSpec(
            num_scalar_prefetch=1,
            grid=(columns // block,),
            in_specs=[
                pl.BlockSpec((depth, block), lambda j, me: (0, j)),
                pl.BlockSpec((rank, depth), lambda j, me: (0, 0)),
                pl.BlockSpec((rank, block), lambda j, me: (0, j)),
            ],
            out_specs=[
                pl.BlockSpec((block, depth), lambda j, me: (j, 0)),
                pl.BlockSpec((block, depth), lambda j, me: (j, me[0])),
            ],
        ),
        out_shape=[
            jax.ShapeDtypeStruct((columns, depth), jnp.bfloat16),
            jax.ShapeDtypeStruct((columns, total), jnp.bfloat16),
        ],
        cost_estimate=cost(columns, depth, rank),
        name="merge",
    )(me, weight, low_t, high)


def source_of(me, n, r, parity):
    forth = lax.rem(me + parity, 2) == 0
    return lax.rem(jnp.where(forth, me + r, me + n - r), n)


def place_kernel(n, hops, staged, me_ref, *refs):
    chunk_refs, refs = refs[: len(hops)], refs[-3:] if staged else (*refs[-2:], None)
    out_ref, sem, stage = refs

    for (r, parity), chunk_ref in zip(hops, chunk_refs):
        held = chunk_ref
        if staged:
            held = stage
            copy = pltpu.make_async_copy(chunk_ref, held, sem.at[1])
            copy.start()
            copy.wait()
        depth = chunk_ref.shape[1]
        column = pl.multiple_of(source_of(me_ref[0], n, r, parity) * depth, 128)
        copy = pltpu.make_async_copy(held, out_ref.at[:, pl.ds(column, depth)], sem.at[0])
        copy.start()
        copy.wait()


def place(me, n, hops, chunks, out, staged):
    rows, depth = chunks[0].shape
    scratch = [pltpu.SemaphoreType.DMA((2,))]
    specs = [pl.BlockSpec(memory_space=pl.ANY if staged else pltpu.VMEM)] * len(hops)
    if staged:
        scratch.append(pltpu.VMEM((rows, depth), jnp.bfloat16))
    else:
        chunks = [pltpu.with_memory_space_constraint(chunk, pltpu.VMEM) for chunk in chunks]
    operands, aliases = [me, *chunks], {}
    if isinstance(out, jax.Array):
        aliases = {len(operands): 0}
        operands.append(out)
        specs.append(pl.BlockSpec(memory_space=pl.ANY))
    return pl.pallas_call(
        functools.partial(place_kernel, n, hops, staged),
        grid_spec=pltpu.PrefetchScalarGridSpec(
            num_scalar_prefetch=1,
            grid=(1,),
            in_specs=specs,
            out_specs=pl.BlockSpec(memory_space=pl.ANY),
            scratch_shapes=scratch,
        ),
        out_shape=jax.ShapeDtypeStruct(out.shape, out.dtype),
        input_output_aliases=aliases,
        cost_estimate=pl.CostEstimate(
            flops=rows * depth, bytes_accessed=4 * rows * depth, transcendentals=0
        ),
        name="place",
    )(*operands)


def hops_of(n):
    return [(1 + i // 2, i % 2) for i in range(n - 1)]


def hop_pairs(n, parity):
    pairs = []
    for i in range(parity, n, 2):
        j = (i + 1) % n
        pairs += [(i, j), (j, i)]
    return pairs


def steps_of(n):
    hops = hops_of(n)
    steps = []
    for chunk in (FIRST, QUERY, LAST):
        steps.append(("merge", None, chunk))
        steps += [("hop", hop, chunk) for hop in hops[:2]]
        if chunk == QUERY:
            steps.append(("place", ((0, 0),), FIRST))
    steps.append(("exchange", None, NORM))
    steps += [("shift", k, NORM) for k in range(1, n)]
    placed = 0
    end = max(len(hops), 2)
    for i in range(2, end + 1):
        for chunk in (FIRST, QUERY, LAST):
            if i == end and chunk == LAST:
                steps.append(("norm", None, NORM))
            steps += [("hop", hop, chunk) for hop in hops[i : i + 1]]
            steps.append(("place", tuple(hops[placed:i]), chunk))
        placed = i
    return steps


def ordered(shifted, me, n):
    parts = []
    for j in range(n):
        part = shifted[0]
        for k in range(1, n):
            part = jnp.where(me == (j + k) % n, shifted[k], part)
        parts.append(part)
    return parts


def gathered(arrays, norm_train, norm_step):
    serve = [
        lax.all_gather(
            (
                weight.astype(jnp.float32)
                + mix_rate * jnp.dot(low, high, preferred_element_type=jnp.float32)
            ).astype(jnp.bfloat16),
            "shard",
            axis=0,
            tiled=True,
        ).T
        for weight, low, high in arrays
    ]
    share = (norm_train + norm_step).astype(jnp.bfloat16)
    return (*serve, lax.all_gather(share, ("shard", "tp"), axis=0, tiled=True))


def solution(mesh):
    n, nt = mesh.shape["shard"], mesh.shape["tp"]
    steps = steps_of(n)

    def on_device(
        weight_query,
        low_query,
        high_query,
        weight_key,
        low_key,
        high_key,
        weight_value,
        low_value,
        high_value,
        norm_train,
        norm_step,
    ):
        depth = weight_query.shape[0]
        weights = (weight_query, weight_key, weight_value)
        if n % 2 or depth % 128 or any(weight.shape[1] % 128 for weight in weights):
            arrays = (
                (weight_query, low_query, high_query),
                (weight_key, low_key, high_key),
                (weight_value, low_value, high_value),
            )
            return gathered(arrays, norm_train, norm_step)
        me = lax.axis_index("shard")
        me_ref = jnp.reshape(me, (1,)).astype(jnp.int32)
        mine = lax.axis_index("tp")
        inputs = {
            KEY: (weight_key, low_key.T, high_key),
            QUERY: (weight_query, low_query.T, high_query),
            VALUE: (weight_value, low_value.T, high_value),
        }
        outs = {}
        got = {}
        for what, hop, chunk in steps:
            if what == "merge":
                if chunk == FIRST:
                    piece = merge_first(*inputs[chunk])
                    outs[chunk] = jax.ShapeDtypeStruct((piece.shape[0], depth * n), piece.dtype)
                else:
                    piece, outs[chunk] = merge(me_ref, *inputs[chunk], depth * n)
                got[(0, 0), chunk] = got[(0, 1), chunk] = piece
            elif what == "hop":
                r, parity = hop
                held = got[(r - 1, 1 - parity), chunk]
                got[hop, chunk] = lax.ppermute(held, "shard", hop_pairs(n, parity))
            elif what == "place":
                pieces = [got[pair, chunk] for pair in hop]
                ends = hop[-1] == hops_of(n)[-1] and chunk == LAST
                staged = not (hop[0] == (0, 0) or ends)
                outs[chunk] = place(me_ref, n, hop, pieces, outs[chunk], staged)
            elif what == "exchange":
                share = (norm_train + norm_step).astype(jnp.bfloat16)
                shares = [share] + [
                    lax.ppermute(share, "tp", [(j, (j + k) % nt) for j in range(nt)])
                    for k in range(1, nt)
                ]
                rows = [jnp.concatenate(ordered(shares, mine, nt))]
            elif what == "shift":
                rows.append(lax.ppermute(rows[0], "shard", [(j, (j + hop) % n) for j in range(n)]))
            else:
                serve_norm = jnp.concatenate(ordered(rows, me, n))
        return outs[QUERY], outs[KEY], outs[VALUE], serve_norm

    in_specs = (
        P(("trial", "shard"), "tp"),
        P(("trial", "shard"), None),
        P("trial", "tp"),
        P(("trial", "shard"), "tp"),
        P(("trial", "shard"), None),
        P("trial", "tp"),
        P(("trial", "shard"), "tp"),
        P(("trial", "shard"), None),
        P("trial", "tp"),
        P(("trial", "shard", "tp")),
        P(("trial", "shard", "tp")),
    )
    out_specs = (
        P(("trial", "tp"), None),
        P(("trial", "tp"), None),
        P(("trial", "tp"), None),
        P("trial"),
    )
    return jax.shard_map(
        on_device, mesh=mesh, in_specs=in_specs, out_specs=out_specs, check_vma=False
    )
```

```python
import functools

import jax
import jax.numpy as jnp
from jax import lax
from jax.experimental import pallas as pl
from jax.experimental.pallas import tpu as pltpu
from jax.sharding import PartitionSpec as P

mix_rate = 1.0


KEY, QUERY, VALUE = range(3)
EIGHTHS = 8
LEAD, KEY_REST = (KEY, 0, 4), (KEY, 4, 4)
QUERY_ALL = (QUERY, 0, 8)
NORM = None
VALUE_REST, LAST = (VALUE, 0, 6), (VALUE, 6, 2)
CHUNKS = (LEAD, KEY_REST, QUERY_ALL, VALUE_REST, LAST)


def extent(columns, chunk):
    return columns * chunk[1] // EIGHTHS, columns * chunk[2] // EIGHTHS


def merged(weight_ref, low_ref, high_ref):
    delta = lax.dot_general(
        high_ref[...], low_ref[...], (((0,), (0,)), ((), ())), preferred_element_type=jnp.float32
    )
    fresh = weight_ref[...].T.astype(jnp.float32) + mix_rate * delta
    return fresh.astype(jnp.bfloat16)


def first_kernel(start, weight_ref, low_ref, high_ref, chunk_ref, weight, low, high, sem):
    columns = pl.ds(start, chunk_ref.shape[0])
    copies = [
        pltpu.make_async_copy(weight_ref.at[:, columns], weight, sem.at[0]),
        pltpu.make_async_copy(low_ref, low, sem.at[1]),
        pltpu.make_async_copy(high_ref.at[:, columns], high, sem.at[2]),
    ]
    for copy in copies:
        copy.start()
    for copy in copies:
        copy.wait()
    chunk_ref[...] = merged(weight, low, high)


def merge_kernel(me_ref, weight_ref, low_ref, high_ref, *refs):
    chunk_ref, out_ref = refs[-2:]
    fresh = merged(weight_ref, low_ref, high_ref)
    chunk_ref[...] = fresh
    out_ref[...] = fresh


def cost(rows, depth, rank):
    return pl.CostEstimate(
        flops=2 * rows * depth * rank, bytes_accessed=6 * rows * depth, transcendentals=0
    )


def merge_first(weight, low_t, high, start, rows):
    depth, rank = weight.shape[0], high.shape[0]
    return pl.pallas_call(
        functools.partial(first_kernel, start),
        in_specs=[pl.BlockSpec(memory_space=pl.ANY)] * 3,
        out_specs=pl.BlockSpec(memory_space=pltpu.VMEM),
        out_shape=pltpu.VMEM((rows, depth), jnp.bfloat16),
        scratch_shapes=[
            pltpu.VMEM((depth, rows), jnp.bfloat16),
            pltpu.VMEM((rank, depth), jnp.bfloat16),
            pltpu.VMEM((rank, rows), jnp.bfloat16),
            pltpu.SemaphoreType.DMA((3,)),
        ],
        cost_estimate=cost(rows, depth, rank),
        name="merge",
    )(weight, low_t, high)


def merge(me, weight, low_t, high, chunk, out):
    depth, columns = weight.shape
    rank = high.shape[0]
    start, rows = extent(columns, chunk)
    block = next(b for b in (512, 384, 256, 128) if start % b == 0 and rows % b == 0)
    first = start // block
    specs = [
        pl.BlockSpec((depth, block), lambda j, me: (0, first + j)),
        pl.BlockSpec((rank, depth), lambda j, me: (0, 0)),
        pl.BlockSpec((rank, block), lambda j, me: (0, first + j)),
    ]
    operands, aliases = [me, weight, low_t, high], {}
    if isinstance(out, jax.Array):
        specs.append(pl.BlockSpec(memory_space=pl.ANY))
        operands.append(out)
        aliases = {4: 1}
    return pl.pallas_call(
        merge_kernel,
        grid_spec=pltpu.PrefetchScalarGridSpec(
            num_scalar_prefetch=1,
            grid=(rows // block,),
            in_specs=specs,
            out_specs=[
                pl.BlockSpec((block, depth), lambda j, me: (j, 0)),
                pl.BlockSpec((block, depth), lambda j, me: (first + j, me[0])),
            ],
        ),
        out_shape=[
            jax.ShapeDtypeStruct((rows, depth), jnp.bfloat16),
            jax.ShapeDtypeStruct(out.shape, jnp.bfloat16),
        ],
        input_output_aliases=aliases,
        cost_estimate=cost(rows, depth, rank),
        name="merge",
    )(*operands)


def source_of(me, n, r, parity):
    forth = lax.rem(me + parity, 2) == 0
    return lax.rem(jnp.where(forth, me + r, me + n - r), n)


def place_kernel(n, hops, start, staged, me_ref, *refs):
    chunk_refs, refs = refs[: len(hops)], refs[-3:] if staged else (*refs[-2:], None)
    out_ref, sem, stage = refs

    for (r, parity), chunk_ref in zip(hops, chunk_refs):
        held = chunk_ref
        if staged:
            held = stage
            copy = pltpu.make_async_copy(chunk_ref, held, sem.at[1])
            copy.start()
            copy.wait()
        rows, depth = chunk_ref.shape
        column = pl.multiple_of(source_of(me_ref[0], n, r, parity) * depth, 128)
        there = out_ref.at[pl.ds(start, rows), pl.ds(column, depth)]
        copy = pltpu.make_async_copy(held, there, sem.at[0])
        copy.start()
        copy.wait()


def place(me, n, hops, chunks, out, start, staged):
    rows, depth = chunks[0].shape
    scratch = [pltpu.SemaphoreType.DMA((2,))]
    specs = [pl.BlockSpec(memory_space=pl.ANY if staged else pltpu.VMEM)] * len(hops)
    if staged:
        scratch.append(pltpu.VMEM((rows, depth), jnp.bfloat16))
    else:
        chunks = [pltpu.with_memory_space_constraint(chunk, pltpu.VMEM) for chunk in chunks]
    operands, aliases = [me, *chunks], {}
    if isinstance(out, jax.Array):
        aliases = {len(operands): 0}
        operands.append(out)
        specs.append(pl.BlockSpec(memory_space=pl.ANY))
    return pl.pallas_call(
        functools.partial(place_kernel, n, hops, start, staged),
        grid_spec=pltpu.PrefetchScalarGridSpec(
            num_scalar_prefetch=1,
            grid=(1,),
            in_specs=specs,
            out_specs=pl.BlockSpec(memory_space=pl.ANY),
            scratch_shapes=scratch,
        ),
        out_shape=jax.ShapeDtypeStruct(out.shape, out.dtype),
        input_output_aliases=aliases,
        cost_estimate=pl.CostEstimate(
            flops=rows * depth, bytes_accessed=4 * rows * depth, transcendentals=0
        ),
        name="place",
    )(*operands)


def hops_of(n):
    return [(1 + i // 2, i % 2) for i in range(n - 1)]


def hop_pairs(n, parity):
    pairs = []
    for i in range(parity, n, 2):
        j = (i + 1) % n
        pairs += [(i, j), (j, i)]
    return pairs


def steps_of(n):
    hops = hops_of(n)
    steps = []
    for chunk in (LEAD, KEY_REST):
        steps += [("merge", None, chunk)] + [("hop", hop, chunk) for hop in hops[:1]]
    steps += [("hop", hop, chunk) for hop in hops[1:2] for chunk in (LEAD, KEY_REST)]
    for chunk in (QUERY_ALL, VALUE_REST, LAST):
        steps += [("merge", None, chunk)] + [("hop", hop, chunk) for hop in hops[:2]]
        if chunk == QUERY_ALL:
            steps += [("place", ((0, 0),), part) for part in (LEAD, KEY_REST)]
    steps.append(("exchange", None, NORM))
    steps += [("shift", k, NORM) for k in range(1, n)]
    placed = 0
    end = max(len(hops), 2)
    for i in range(2, end + 1):
        for chunk in CHUNKS:
            if i == end and chunk == LAST:
                steps.append(("norm", None, NORM))
            steps += [("hop", hop, chunk) for hop in hops[i : i + 1]]
            steps.append(("place", tuple(hops[placed:i]), chunk))
        placed = i
    return steps


def ordered(shifted, me, n):
    parts = []
    for j in range(n):
        part = shifted[0]
        for k in range(1, n):
            part = jnp.where(me == (j + k) % n, shifted[k], part)
        parts.append(part)
    return parts


def gathered(arrays, norm_train, norm_step):
    serve = [
        lax.all_gather(
            (
                weight.astype(jnp.float32)
                + mix_rate * jnp.dot(low, high, preferred_element_type=jnp.float32)
            ).astype(jnp.bfloat16),
            "shard",
            axis=0,
            tiled=True,
        ).T
        for weight, low, high in arrays
    ]
    share = (norm_train + norm_step).astype(jnp.bfloat16)
    return (*serve, lax.all_gather(share, ("shard", "tp"), axis=0, tiled=True))


def solution(mesh):
    n, nt = mesh.shape["shard"], mesh.shape["tp"]
    steps = steps_of(n)

    def on_device(
        weight_query,
        low_query,
        high_query,
        weight_key,
        low_key,
        high_key,
        weight_value,
        low_value,
        high_value,
        norm_train,
        norm_step,
    ):
        depth = weight_query.shape[0]
        weights = (weight_query, weight_key, weight_value)
        if n % 2 or depth % 128 or any(weight.shape[1] % 512 for weight in weights):
            arrays = (
                (weight_query, low_query, high_query),
                (weight_key, low_key, high_key),
                (weight_value, low_value, high_value),
            )
            return gathered(arrays, norm_train, norm_step)
        me = lax.axis_index("shard")
        me_ref = jnp.reshape(me, (1,)).astype(jnp.int32)
        mine = lax.axis_index("tp")
        inputs = {
            KEY: (weight_key, low_key.T, high_key),
            QUERY: (weight_query, low_query.T, high_query),
            VALUE: (weight_value, low_value.T, high_value),
        }
        outs = {}
        got = {}
        for what, hop, chunk in steps:
            if what == "merge":
                which = chunk[0]
                columns = inputs[which][0].shape[1]
                whole = jax.ShapeDtypeStruct((columns, depth * n), jnp.bfloat16)
                out = outs.setdefault(which, whole)
                if which == KEY:
                    piece = merge_first(*inputs[which], *extent(columns, chunk))
                else:
                    piece, outs[which] = merge(me_ref, *inputs[which], chunk, out)
                got[(0, 0), chunk] = got[(0, 1), chunk] = piece
            elif what == "hop":
                r, parity = hop
                held = got[(r - 1, 1 - parity), chunk]
                got[hop, chunk] = lax.ppermute(held, "shard", hop_pairs(n, parity))
            elif what == "place":
                pieces = [got[pair, chunk] for pair in hop]
                ends = hop[-1] == hops_of(n)[-1] and chunk[0] == VALUE
                staged = not (hop[0] == (0, 0) or ends)
                out = outs[chunk[0]]
                start, _ = extent(out.shape[0], chunk)
                outs[chunk[0]] = place(me_ref, n, hop, pieces, out, start, staged)
            elif what == "exchange":
                share = (norm_train + norm_step).astype(jnp.bfloat16)
                shares = [share] + [
                    lax.ppermute(share, "tp", [(j, (j + k) % nt) for j in range(nt)])
                    for k in range(1, nt)
                ]
                rows = [jnp.concatenate(ordered(shares, mine, nt))]
            elif what == "shift":
                rows.append(lax.ppermute(rows[0], "shard", [(j, (j + hop) % n) for j in range(n)]))
            else:
                serve_norm = jnp.concatenate(ordered(rows, me, n))
        return outs[QUERY], outs[KEY], outs[VALUE], serve_norm

    in_specs = (
        P(("trial", "shard"), "tp"),
        P(("trial", "shard"), None),
        P("trial", "tp"),
        P(("trial", "shard"), "tp"),
        P(("trial", "shard"), None),
        P("trial", "tp"),
        P(("trial", "shard"), "tp"),
        P(("trial", "shard"), None),
        P("trial", "tp"),
        P(("trial", "shard", "tp")),
        P(("trial", "shard", "tp")),
    )
    out_specs = (
        P(("trial", "tp"), None),
        P(("trial", "tp"), None),
        P(("trial", "tp"), None),
        P("trial"),
    )
    return jax.shard_map(
        on_device, mesh=mesh, in_specs=in_specs, out_specs=out_specs, check_vma=False
    )
```

```python
import functools

import jax
import jax.numpy as jnp
from jax import lax
from jax.experimental import pallas as pl
from jax.experimental.pallas import tpu as pltpu
from jax.sharding import PartitionSpec as P

mix_rate = 1.0


KEY, QUERY, VALUE = range(3)
EIGHTHS = 8
LEAD, KEY_REST = (KEY, 0, 4), (KEY, 4, 4)
QUERY_ALL = (QUERY, 0, 8)
NORM = None
VALUE_REST, LAST = (VALUE, 0, 6), (VALUE, 6, 2)
CHUNKS = (LEAD, KEY_REST, QUERY_ALL, VALUE_REST, LAST)


def extent(columns, chunk):
    return columns * chunk[1] // EIGHTHS, columns * chunk[2] // EIGHTHS


def merged(weight_ref, low_ref, high_ref):
    delta = lax.dot_general(
        high_ref[...], low_ref[...], (((0,), (0,)), ((), ())), preferred_element_type=jnp.float32
    )
    fresh = weight_ref[...].T.astype(jnp.float32) + mix_rate * delta
    return fresh.astype(jnp.bfloat16)


def first_kernel(start, weight_ref, low_ref, high_ref, chunk_ref, weight, low, high, sem):
    columns = pl.ds(start, chunk_ref.shape[0])
    copies = [
        pltpu.make_async_copy(weight_ref.at[:, columns], weight, sem.at[0]),
        pltpu.make_async_copy(low_ref, low, sem.at[1]),
        pltpu.make_async_copy(high_ref.at[:, columns], high, sem.at[2]),
    ]
    for copy in copies:
        copy.start()
    for copy in copies:
        copy.wait()
    chunk_ref[...] = merged(weight, low, high)


def merge_kernel(me_ref, weight_ref, low_ref, high_ref, *refs):
    chunk_ref, out_ref = refs[-2:]
    fresh = merged(weight_ref, low_ref, high_ref)
    chunk_ref[...] = fresh
    out_ref[...] = fresh


def cost(rows, depth, rank):
    return pl.CostEstimate(
        flops=2 * rows * depth * rank, bytes_accessed=6 * rows * depth, transcendentals=0
    )


def merge_first(weight, low_t, high, start, rows):
    depth, rank = weight.shape[0], high.shape[0]
    return pl.pallas_call(
        functools.partial(first_kernel, start),
        in_specs=[pl.BlockSpec(memory_space=pl.ANY)] * 3,
        out_specs=pl.BlockSpec(memory_space=pltpu.VMEM),
        out_shape=pltpu.VMEM((rows, depth), jnp.bfloat16),
        scratch_shapes=[
            pltpu.VMEM((depth, rows), jnp.bfloat16),
            pltpu.VMEM((rank, depth), jnp.bfloat16),
            pltpu.VMEM((rank, rows), jnp.bfloat16),
            pltpu.SemaphoreType.DMA((3,)),
        ],
        cost_estimate=cost(rows, depth, rank),
        name="merge",
    )(weight, low_t, high)


def merge(me, weight, low_t, high, chunk, out):
    depth, columns = weight.shape
    rank = high.shape[0]
    start, rows = extent(columns, chunk)
    block = next(b for b in (512, 384, 256, 128) if start % b == 0 and rows % b == 0)
    first = start // block
    specs = [
        pl.BlockSpec((depth, block), lambda j, me: (0, first + j)),
        pl.BlockSpec((rank, depth), lambda j, me: (0, 0)),
        pl.BlockSpec((rank, block), lambda j, me: (0, first + j)),
    ]
    operands, aliases = [me, weight, low_t, high], {}
    if isinstance(out, jax.Array):
        specs.append(pl.BlockSpec(memory_space=pl.ANY))
        operands.append(out)
        aliases = {4: 1}
    return pl.pallas_call(
        merge_kernel,
        grid_spec=pltpu.PrefetchScalarGridSpec(
            num_scalar_prefetch=1,
            grid=(rows // block,),
            in_specs=specs,
            out_specs=[
                pl.BlockSpec((block, depth), lambda j, me: (j, 0)),
                pl.BlockSpec((block, depth), lambda j, me: (first + j, me[0])),
            ],
        ),
        out_shape=[
            jax.ShapeDtypeStruct((rows, depth), jnp.bfloat16),
            jax.ShapeDtypeStruct(out.shape, jnp.bfloat16),
        ],
        input_output_aliases=aliases,
        cost_estimate=cost(rows, depth, rank),
        name="merge",
    )(*operands)


def source_of(me, n, r, parity):
    forth = lax.rem(me + parity, 2) == 0
    return lax.rem(jnp.where(forth, me + r, me + n - r), n)


def place_kernel(n, hops, start, staged, *refs):
    chunk_refs, refs = refs[: len(hops)], refs[-3:] if staged else (*refs[-2:], None)
    out_ref, sem, stage = refs
    me = lax.axis_index("shard")

    for (r, parity), chunk_ref in zip(hops, chunk_refs):
        held = chunk_ref
        if staged:
            held = stage
            copy = pltpu.make_async_copy(chunk_ref, held, sem.at[1])
            copy.start()
            copy.wait()
        rows, depth = chunk_ref.shape
        column = pl.multiple_of(source_of(me, n, r, parity) * depth, 128)
        there = out_ref.at[pl.ds(start, rows), pl.ds(column, depth)]
        copy = pltpu.make_async_copy(held, there, sem.at[0])
        copy.start()
        copy.wait()


def place(n, hops, chunks, out, start, staged):
    rows, depth = chunks[0].shape
    scratch = [pltpu.SemaphoreType.DMA((2,))]
    specs = [pl.BlockSpec(memory_space=pl.ANY if staged else pltpu.VMEM)] * len(hops)
    if staged:
        scratch.append(pltpu.VMEM((rows, depth), jnp.bfloat16))
    else:
        chunks = [pltpu.with_memory_space_constraint(chunk, pltpu.VMEM) for chunk in chunks]
    operands, aliases = [*chunks], {}
    if isinstance(out, jax.Array):
        aliases = {len(operands): 0}
        operands.append(out)
        specs.append(pl.BlockSpec(memory_space=pl.ANY))
    return pl.pallas_call(
        functools.partial(place_kernel, n, hops, start, staged),
        in_specs=specs,
        out_specs=pl.BlockSpec(memory_space=pl.ANY),
        scratch_shapes=scratch,
        out_shape=jax.ShapeDtypeStruct(out.shape, out.dtype),
        input_output_aliases=aliases,
        cost_estimate=pl.CostEstimate(
            flops=rows * depth, bytes_accessed=4 * rows * depth, transcendentals=0
        ),
        name="place",
    )(*operands)


def hops_of(n):
    return [(1 + i // 2, i % 2) for i in range(n - 1)]


def hop_pairs(n, parity):
    pairs = []
    for i in range(parity, n, 2):
        j = (i + 1) % n
        pairs += [(i, j), (j, i)]
    return pairs


def steps_of(n):
    hops = hops_of(n)
    steps = []
    for chunk in (LEAD, KEY_REST):
        steps += [("merge", None, chunk)] + [("hop", hop, chunk) for hop in hops[:1]]
    steps += [("hop", hop, chunk) for hop in hops[1:2] for chunk in (LEAD, KEY_REST)]
    for chunk in (QUERY_ALL, VALUE_REST, LAST):
        steps += [("merge", None, chunk)] + [("hop", hop, chunk) for hop in hops[:2]]
        if chunk == QUERY_ALL:
            steps += [("place", ((0, 0),), part) for part in (LEAD, KEY_REST)]
    steps.append(("exchange", None, NORM))
    steps += [("shift", k, NORM) for k in range(1, n)]
    placed = 0
    end = max(len(hops), 2)
    for i in range(2, end + 1):
        for chunk in CHUNKS:
            if i == end and chunk == LAST:
                steps.append(("norm", None, NORM))
            steps += [("hop", hop, chunk) for hop in hops[i : i + 1]]
            steps.append(("place", tuple(hops[placed:i]), chunk))
        placed = i
    return steps


def ordered(shifted, me, n):
    parts = []
    for j in range(n):
        part = shifted[0]
        for k in range(1, n):
            part = jnp.where(me == (j + k) % n, shifted[k], part)
        parts.append(part)
    return parts


def gathered(arrays, norm_train, norm_step):
    serve = [
        lax.all_gather(
            (
                weight.astype(jnp.float32)
                + mix_rate * jnp.dot(low, high, preferred_element_type=jnp.float32)
            ).astype(jnp.bfloat16),
            "shard",
            axis=0,
            tiled=True,
        ).T
        for weight, low, high in arrays
    ]
    share = (norm_train + norm_step).astype(jnp.bfloat16)
    return (*serve, lax.all_gather(share, ("shard", "tp"), axis=0, tiled=True))


def solution(mesh):
    n, nt = mesh.shape["shard"], mesh.shape["tp"]
    steps = steps_of(n)

    def on_device(
        weight_query,
        low_query,
        high_query,
        weight_key,
        low_key,
        high_key,
        weight_value,
        low_value,
        high_value,
        norm_train,
        norm_step,
    ):
        depth = weight_query.shape[0]
        weights = (weight_query, weight_key, weight_value)
        if n % 2 or depth % 128 or any(weight.shape[1] % 512 for weight in weights):
            arrays = (
                (weight_query, low_query, high_query),
                (weight_key, low_key, high_key),
                (weight_value, low_value, high_value),
            )
            return gathered(arrays, norm_train, norm_step)
        me = lax.axis_index("shard")
        me_ref = jnp.reshape(me, (1,)).astype(jnp.int32)
        mine = lax.axis_index("tp")
        inputs = {
            KEY: (weight_key, low_key.T, high_key),
            QUERY: (weight_query, low_query.T, high_query),
            VALUE: (weight_value, low_value.T, high_value),
        }
        outs = {}
        got = {}
        for what, hop, chunk in steps:
            if what == "merge":
                which = chunk[0]
                columns = inputs[which][0].shape[1]
                whole = jax.ShapeDtypeStruct((columns, depth * n), jnp.bfloat16)
                out = outs.setdefault(which, whole)
                if which == KEY:
                    piece = merge_first(*inputs[which], *extent(columns, chunk))
                else:
                    piece, outs[which] = merge(me_ref, *inputs[which], chunk, out)
                got[(0, 0), chunk] = got[(0, 1), chunk] = piece
            elif what == "hop":
                r, parity = hop
                held = got[(r - 1, 1 - parity), chunk]
                got[hop, chunk] = lax.ppermute(held, "shard", hop_pairs(n, parity))
            elif what == "place":
                pieces = [got[pair, chunk] for pair in hop]
                ends = hop[-1] == hops_of(n)[-1] and chunk[0] == VALUE
                staged = not (hop[0] == (0, 0) or ends)
                out = outs[chunk[0]]
                start, _ = extent(out.shape[0], chunk)
                outs[chunk[0]] = place(n, hop, pieces, out, start, staged)
            elif what == "exchange":
                share = (norm_train + norm_step).astype(jnp.bfloat16)
                shares = [share] + [
                    lax.ppermute(share, "tp", [(j, (j + k) % nt) for j in range(nt)])
                    for k in range(1, nt)
                ]
                rows = [jnp.concatenate(ordered(shares, mine, nt))]
            elif what == "shift":
                rows.append(lax.ppermute(rows[0], "shard", [(j, (j + hop) % n) for j in range(n)]))
            else:
                serve_norm = jnp.concatenate(ordered(rows, me, n))
        return outs[QUERY], outs[KEY], outs[VALUE], serve_norm

    in_specs = (
        P(("trial", "shard"), "tp"),
        P(("trial", "shard"), None),
        P("trial", "tp"),
        P(("trial", "shard"), "tp"),
        P(("trial", "shard"), None),
        P("trial", "tp"),
        P(("trial", "shard"), "tp"),
        P(("trial", "shard"), None),
        P("trial", "tp"),
        P(("trial", "shard", "tp")),
        P(("trial", "shard", "tp")),
    )
    out_specs = (
        P(("trial", "tp"), None),
        P(("trial", "tp"), None),
        P(("trial", "tp"), None),
        P("trial"),
    )
    return jax.shard_map(
        on_device, mesh=mesh, in_specs=in_specs, out_specs=out_specs, check_vma=False
    )
```

```python
import functools

import jax
import jax.numpy as jnp
from jax import lax
from jax.experimental import pallas as pl
from jax.experimental.pallas import tpu as pltpu
from jax.sharding import PartitionSpec as P

mix_rate = 1.0


KEY, QUERY, VALUE = range(3)
EIGHTHS = 8
LEAD, KEY_REST, KEY_ALL = (KEY, 0, 4), (KEY, 4, 4), (KEY, 0, 8)
QUERY_ALL = (QUERY, 0, 8)
NORM = None
VALUE_ALL, VALUE_REST, LAST = (VALUE, 0, 8), (VALUE, 0, 6), (VALUE, 6, 2)


def extent(columns, chunk):
    return columns * chunk[1] // EIGHTHS, columns * chunk[2] // EIGHTHS


def merged(weight_ref, low_ref, high_ref):
    delta = lax.dot_general(
        high_ref[...], low_ref[...], (((0,), (0,)), ((), ())), preferred_element_type=jnp.float32
    )
    fresh = weight_ref[...].T.astype(jnp.float32) + mix_rate * delta
    return fresh.astype(jnp.bfloat16)


def first_kernel(start, weight_ref, low_ref, high_ref, chunk_ref, weight, low, high, sem):
    columns = pl.ds(start, chunk_ref.shape[0])
    copies = [
        pltpu.make_async_copy(weight_ref.at[:, columns], weight, sem.at[0]),
        pltpu.make_async_copy(low_ref, low, sem.at[1]),
        pltpu.make_async_copy(high_ref.at[:, columns], high, sem.at[2]),
    ]
    for copy in copies:
        copy.start()
    for copy in copies:
        copy.wait()
    chunk_ref[...] = merged(weight, low, high)


def merge_kernel(me_ref, weight_ref, low_ref, high_ref, *refs):
    chunk_ref, out_ref = refs[-2:]
    fresh = merged(weight_ref, low_ref, high_ref)
    chunk_ref[...] = fresh
    out_ref[...] = fresh


def cost(rows, depth, rank):
    return pl.CostEstimate(
        flops=2 * rows * depth * rank, bytes_accessed=6 * rows * depth, transcendentals=0
    )


def merge_first(weight, low_t, high, start, rows):
    depth, rank = weight.shape[0], high.shape[0]
    return pl.pallas_call(
        functools.partial(first_kernel, start),
        in_specs=[pl.BlockSpec(memory_space=pl.ANY)] * 3,
        out_specs=pl.BlockSpec(memory_space=pltpu.VMEM),
        out_shape=pltpu.VMEM((rows, depth), jnp.bfloat16),
        scratch_shapes=[
            pltpu.VMEM((depth, rows), jnp.bfloat16),
            pltpu.VMEM((rank, depth), jnp.bfloat16),
            pltpu.VMEM((rank, rows), jnp.bfloat16),
            pltpu.SemaphoreType.DMA((3,)),
        ],
        cost_estimate=cost(rows, depth, rank),
        name="merge",
    )(weight, low_t, high)


def merge(me, weight, low_t, high, chunk, out):
    depth, columns = weight.shape
    rank = high.shape[0]
    start, rows = extent(columns, chunk)
    block = next(b for b in (256, 128) if start % b == 0 and rows % (4 * b) == 0)
    first = start // block
    specs = [
        pl.BlockSpec((depth, block), lambda j, me: (0, first + j)),
        pl.BlockSpec((rank, depth), lambda j, me: (0, 0)),
        pl.BlockSpec((rank, block), lambda j, me: (0, first + j)),
    ]
    operands, aliases = [me, weight, low_t, high], {}
    if isinstance(out, jax.Array):
        specs.append(pl.BlockSpec(memory_space=pl.ANY))
        operands.append(out)
        aliases = {4: 1}
    return pl.pallas_call(
        merge_kernel,
        grid_spec=pltpu.PrefetchScalarGridSpec(
            num_scalar_prefetch=1,
            grid=(rows // block,),
            in_specs=specs,
            out_specs=[
                pl.BlockSpec((block, depth), lambda j, me: (j, 0)),
                pl.BlockSpec((block, depth), lambda j, me: (first + j, me[0])),
            ],
        ),
        out_shape=[
            jax.ShapeDtypeStruct((rows, depth), jnp.bfloat16),
            jax.ShapeDtypeStruct(out.shape, jnp.bfloat16),
        ],
        input_output_aliases=aliases,
        cost_estimate=cost(rows, depth, rank),
        name="merge",
    )(*operands)


def source_of(me, n, r, parity):
    forth = lax.rem(me + parity, 2) == 0
    return lax.rem(jnp.where(forth, me + r, me + n - r), n)


def place_kernel(n, hops, start, staged, me_ref, *refs):
    chunk_refs, refs = refs[: len(hops)], refs[-3:] if staged else (*refs[-2:], None)
    out_ref, sem, stage = refs

    for (r, parity), chunk_ref in zip(hops, chunk_refs):
        held = chunk_ref
        if staged:
            held = stage
            copy = pltpu.make_async_copy(chunk_ref, held, sem.at[1])
            copy.start()
            copy.wait()
        rows, depth = chunk_ref.shape
        column = pl.multiple_of(source_of(me_ref[0], n, r, parity) * depth, 128)
        there = out_ref.at[pl.ds(start, rows), pl.ds(column, depth)]
        copy = pltpu.make_async_copy(held, there, sem.at[0])
        copy.start()
        copy.wait()


def place(me, n, hops, chunks, out, start, staged):
    rows, depth = chunks[0].shape
    scratch = [pltpu.SemaphoreType.DMA((2,))]
    specs = [pl.BlockSpec(memory_space=pl.ANY if staged else pltpu.VMEM)] * len(hops)
    if staged:
        scratch.append(pltpu.VMEM((rows, depth), jnp.bfloat16))
    else:
        chunks = [pltpu.with_memory_space_constraint(chunk, pltpu.VMEM) for chunk in chunks]
    operands, aliases = [me, *chunks], {}
    if isinstance(out, jax.Array):
        aliases = {len(operands): 0}
        operands.append(out)
        specs.append(pl.BlockSpec(memory_space=pl.ANY))
    return pl.pallas_call(
        functools.partial(place_kernel, n, hops, start, staged),
        grid_spec=pltpu.PrefetchScalarGridSpec(
            num_scalar_prefetch=1,
            grid=(1,),
            in_specs=specs,
            out_specs=pl.BlockSpec(memory_space=pl.ANY),
            scratch_shapes=scratch,
        ),
        out_shape=jax.ShapeDtypeStruct(out.shape, out.dtype),
        input_output_aliases=aliases,
        cost_estimate=pl.CostEstimate(
            flops=rows * depth, bytes_accessed=4 * rows * depth, transcendentals=0
        ),
        name="place",
    )(*operands)


def hops_of(n):
    return [(1 + i // 2, i % 2) for i in range(n - 1)]


def hop_pairs(n, parity):
    pairs = []
    for i in range(parity, n, 2):
        j = (i + 1) % n
        pairs += [(i, j), (j, i)]
    return pairs


def steps_of(n):
    hops = hops_of(n)
    steps = []
    for chunk in (LEAD, KEY_REST):
        steps += [("merge", None, chunk)] + [("hop", hop, chunk) for hop in hops[:1]]
    steps.append(("join", hops[:1], KEY_ALL))
    steps += [("hop", hop, KEY_ALL) for hop in hops[1:2]]
    for chunk in (QUERY_ALL, VALUE_ALL):
        steps += [("merge", None, chunk)] + [("hop", hop, chunk) for hop in hops[:2]]
        if chunk == QUERY_ALL:
            steps.append(("place", ((0, 0),), KEY_ALL))
    steps.append(("exchange", None, NORM))
    steps += [("shift", k, NORM) for k in range(1, n)]
    placed = 0
    end = max(len(hops), 2)
    for i in range(2, end + 1):
        for chunk in (KEY_ALL, QUERY_ALL, VALUE_ALL):
            if i == end and chunk == VALUE_ALL:
                steps.append(("norm", None, NORM))
            parts = (chunk,)
            if chunk == VALUE_ALL and i == len(hops) - 1:
                steps.append(("split", hops[i], chunk))
                parts = (VALUE_REST, LAST)
            steps += [("hop", hop, part) for hop in hops[i : i + 1] for part in parts]
            parts = (VALUE_REST, LAST) if chunk == VALUE_ALL and i == end > 2 else (chunk,)
            steps += [("place", tuple(hops[placed:i]), part) for part in parts]
        placed = i
    return steps


def ordered(shifted, me, n):
    parts = []
    for j in range(n):
        part = shifted[0]
        for k in range(1, n):
            part = jnp.where(me == (j + k) % n, shifted[k], part)
        parts.append(part)
    return parts


def gathered(arrays, norm_train, norm_step):
    serve = [
        lax.all_gather(
            (
                weight.astype(jnp.float32)
                + mix_rate * jnp.dot(low, high, preferred_element_type=jnp.float32)
            ).astype(jnp.bfloat16),
            "shard",
            axis=0,
            tiled=True,
        ).T
        for weight, low, high in arrays
    ]
    share = (norm_train + norm_step).astype(jnp.bfloat16)
    return (*serve, lax.all_gather(share, ("shard", "tp"), axis=0, tiled=True))


def solution(mesh):
    n, nt = mesh.shape["shard"], mesh.shape["tp"]
    steps = steps_of(n)

    def on_device(
        weight_query,
        low_query,
        high_query,
        weight_key,
        low_key,
        high_key,
        weight_value,
        low_value,
        high_value,
        norm_train,
        norm_step,
    ):
        depth = weight_query.shape[0]
        weights = (weight_query, weight_key, weight_value)
        if n % 2 or depth % 128 or any(weight.shape[1] % 512 for weight in weights):
            arrays = (
                (weight_query, low_query, high_query),
                (weight_key, low_key, high_key),
                (weight_value, low_value, high_value),
            )
            return gathered(arrays, norm_train, norm_step)
        me = lax.axis_index("shard")
        me_ref = jnp.reshape(me, (1,)).astype(jnp.int32)
        mine = lax.axis_index("tp")
        inputs = {
            KEY: (weight_key, low_key.T, high_key),
            QUERY: (weight_query, low_query.T, high_query),
            VALUE: (weight_value, low_value.T, high_value),
        }
        outs = {}
        got = {}
        for what, hop, chunk in steps:
            if what == "merge":
                which = chunk[0]
                columns = inputs[which][0].shape[1]
                whole = jax.ShapeDtypeStruct((columns, depth * n), jnp.bfloat16)
                out = outs.setdefault(which, whole)
                if which == KEY:
                    piece = merge_first(*inputs[which], *extent(columns, chunk))
                else:
                    piece, outs[which] = merge(me_ref, *inputs[which], chunk, out)
                got[(0, 0), chunk] = got[(0, 1), chunk] = piece
            elif what == "join":
                for pair in ((0, 0), (0, 1), *hop):
                    parts = [got[pair, LEAD], got[pair, KEY_REST]]
                    got[pair, chunk] = jnp.concatenate(parts)
            elif what == "split":
                r, parity = hop
                held = got[(r - 1, 1 - parity), chunk]
                for part in (VALUE_REST, LAST):
                    start, size = extent(held.shape[0], part)
                    got[(r - 1, 1 - parity), part] = held[start : start + size]
            elif what == "hop":
                r, parity = hop
                held = got[(r - 1, 1 - parity), chunk]
                got[hop, chunk] = lax.ppermute(held, "shard", hop_pairs(n, parity))
            elif what == "place":
                pieces = [got[pair, chunk] for pair in hop]
                ends = hop[-1] == hops_of(n)[-1] and chunk[0] == VALUE
                staged = not (hop[0] == (0, 0) or ends)
                out = outs[chunk[0]]
                start, _ = extent(out.shape[0], chunk)
                outs[chunk[0]] = place(me_ref, n, hop, pieces, out, start, staged)
            elif what == "exchange":
                share = (norm_train + norm_step).astype(jnp.bfloat16)
                shares = [share] + [
                    lax.ppermute(share, "tp", [(j, (j + k) % nt) for j in range(nt)])
                    for k in range(1, nt)
                ]
                rows = [jnp.concatenate(ordered(shares, mine, nt))]
            elif what == "shift":
                rows.append(lax.ppermute(rows[0], "shard", [(j, (j + hop) % n) for j in range(n)]))
            else:
                serve_norm = jnp.concatenate(ordered(rows, me, n))
        return outs[QUERY], outs[KEY], outs[VALUE], serve_norm

    in_specs = (
        P(("trial", "shard"), "tp"),
        P(("trial", "shard"), None),
        P("trial", "tp"),
        P(("trial", "shard"), "tp"),
        P(("trial", "shard"), None),
        P("trial", "tp"),
        P(("trial", "shard"), "tp"),
        P(("trial", "shard"), None),
        P("trial", "tp"),
        P(("trial", "shard", "tp")),
        P(("trial", "shard", "tp")),
    )
    out_specs = (
        P(("trial", "tp"), None),
        P(("trial", "tp"), None),
        P(("trial", "tp"), None),
        P("trial"),
    )
    return jax.shard_map(
        on_device, mesh=mesh, in_specs=in_specs, out_specs=out_specs, check_vma=False
    )
```
